512 devices in a mesh: parts: 2 (over y), rows: 16 (over x, core), cols: 16 (over z).
Axes of the slice: x: 8, y: 2, z: 16, core: 2. Of those that a mesh axis runs over, the one named last changes fastest.
The devices are a block of a 8x16x16 slice.
Arguments:
- singles: bfloat16 [4096, 384], P(('parts', 'rows', 'cols')), parts along dimension 0, may hold values from -120 to 120
- pair: bfloat16 [4096, 2048, 128], P(('parts', 'rows'), 'cols'), parts along dimension 0, may hold values from -6 to 6
- chain_sizes: int32 [16], P('parts'), parts along dimension 0, may hold values from 1 to 512, 2048 in all
- single_proj: bfloat16 [384, 1536], replicated, may hold values from -1 to 1
- query_bias: float32 [384], replicated, may hold values from -5 to 5
- pair_proj: bfloat16 [128, 16], replicated, may hold values from -0.5 to 0.5
- out_proj: bfloat16 [384, 384], replicated, may hold values from -1.25 to 1.25
Outputs:
- update: bfloat16 [4096, 384], P(('parts', 'rows', 'cols')), parts along dimension 0
The draws below stay inside these ranges and needn't reach their ends.
There are 2 independent parts, one for each index of `parts`. The reference program is written for one: setup_inputs(seed, part) draws one part's arguments, and reference() takes and returns one part's arrays. A program takes and returns all parts, laid end to end along the dimension named above; an argument that names none is the same for every part. Nothing has to cross between parts.
Inputs may be any that keep to these rules, and one draw needn't show every extreme that they name: `chain_sizes`: the first 7 entries count the tokens of the chains in order; the last one counts the padding tokens at the end of the complex.
All inputs are finite; a program needn't handle non-finite values.
Results may differ from the reference program's by a relative error of at most 0.004.
The reference program's roundings to bfloat16 on the way (of `normed`, `queries`, `pair_normed`, `pair_bias`, `rounded` and `attended`) count: a program that leaves them out, or rounds other values in their place, can miss the bound.
Values may be sent and summed in bfloat16 or wider, within the bound.
A program may use at most 64 MiB of HBM per device.

```python
import math
import jax
import jax.numpy as jnp
import numpy as np
from jax import lax

C = 384
CZ = 128
H = 16
SLOTS = 8
TOKENS = 2048


def draw_singles(key, part):
    noise = jnp.clip(jax.random.normal(key, (TOKENS, C), jnp.float32), -6.0, 6.0)
    return noise.astype(jnp.bfloat16)


def draw_single_proj(key, part):
    base = jnp.clip(jax.random.normal(key, (C, 4 * C), jnp.float32), -4.0, 4.0) / math.sqrt(C)
    return base.astype(jnp.bfloat16)


def shard_levels(key, shape, pieces, low, largest):
    def one(axis_at, parts):
        steps = jax.random.uniform(jax.random.fold_in(jax.random.fold_in(key, 6), axis_at), (parts,), jnp.float32, low / len(pieces), largest / len(pieces))
        return jnp.repeat(jnp.exp(steps), shape[axis_at] // parts).reshape((-1,) + (1,) * (len(shape) - axis_at - 1))

    gain = one(*pieces[0])
    for cut in pieces[1:]:
        gain = gain * one(*cut)
    return gain


def profile(number_of, total, reach, lean):
    portions = [(1 << 20) // math.isqrt(grade ** lean) + 1 for grade in range(2, number_of + 1)]
    spare, given = total - reach - (number_of - 1), [1] * (number_of - 1)
    while spare > 0:
        free = [i for i in range(number_of - 1) if given[i] < reach]
        whole, left = sum([portions[i] for i in free]), spare
        for i in free:
            more = min(reach - given[i], max(1, left * portions[i] // whole), spare)
            given[i] = given[i] + more
            spare = spare - more
    return np.array([reach] + given)


def uneven(stream_key, count, total, reach, slope):
    if count == 2:
        one = jax.random.randint(stream_key, (), max(1, total - reach), min(reach, total - 1) + 1)
        return jnp.stack([one, total - one])
    lengths = jnp.asarray(profile(count, total, reach, slope), jnp.int32)
    twos = (count - 1) // 2
    donor, sink = lengths[1:1 + 2 * twos:2], lengths[2:2 + 2 * twos:2]
    room = jnp.minimum(donor - 1, reach - sink)
    moved = jax.random.randint(jax.random.fold_in(stream_key, 1), (twos,), 0, 1 << 20) % (room + 1)
    lengths = lengths.at[1:1 + 2 * twos:2].set(donor - moved).at[2:2 + 2 * twos:2].set(sink + moved)
    return lengths[jax.random.permutation(jax.random.fold_in(stream_key, 2), count)]


def centred(stream_key, extent, spread, limit, cuts=(), kind=jnp.bfloat16):
    factor_of = shard_levels(stream_key, extent, cuts, -0.22, 0.18) if cuts else 1.0
    entries = jax.random.normal(stream_key, extent, jnp.float32) * spread * factor_of
    return jnp.minimum(jnp.maximum(entries, -limit), limit).astype(kind)


def setup_inputs(seed: int = 0, part: int = 0) -> dict:
    key_of = jax.random.split(jax.random.key(seed), 8)
    own_keys = jax.random.split(jax.random.fold_in(key_of[7], part), 8)
    singles = draw_singles(jax.random.fold_in(jax.random.fold_in(key_of[7], part), 71), part)
    pair = centred(own_keys[1], (TOKENS, TOKENS, CZ), 1.0, 6.0, ((0, 16), (1, 16)))
    chain_sizes = uneven(own_keys[2], SLOTS, TOKENS, TOKENS // 4, 1).astype(jnp.int32)
    single_proj = draw_single_proj(jax.random.fold_in(key_of[7], 71), part)
    query_bias = centred(key_of[4], (C,), 1.0, 5.0, (), jnp.float32)
    pair_proj = centred(key_of[5], (CZ, H), CZ ** -0.5, 0.5)
    out_proj = centred(key_of[6], (C, C), (C // 16) ** -0.5, 1.25)
    return dict(singles=singles, pair=pair, chain_sizes=chain_sizes, single_proj=single_proj, query_bias=query_bias, pair_proj=pair_proj, out_proj=out_proj)


def normalize(matrix):
    average = lax.optimization_barrier(jnp.mean(matrix, axis=-1, keepdims=True))
    centered = matrix - average
    variance = lax.optimization_barrier(jnp.mean(centered * centered, axis=-1, keepdims=True))
    return centered * lax.rsqrt(variance + 1e-05)

def reference(singles, pair, chain_sizes, single_proj, query_bias, pair_proj, out_proj):
    features = C
    head_dim = C // H
    score_scale = head_dim ** (-0.5)
    normed = normalize(singles.astype(jnp.float32)).astype(jnp.bfloat16)
    projected = jnp.dot(normed, single_proj, preferred_element_type=jnp.float32)
    queries = (projected[:, :features] + query_bias.astype(jnp.float32)).astype(jnp.bfloat16)
    key_rows = projected[:, features:2 * features].astype(jnp.bfloat16)
    values = projected[:, 2 * features:3 * features].astype(jnp.bfloat16)
    gating = jax.nn.sigmoid(projected[:, 3 * features:])
    live_count = jnp.sum(chain_sizes[:-1])
    key_live = jnp.arange(TOKENS, dtype=jnp.int32) < live_count
    key_heads = key_rows.astype(jnp.float32).reshape(TOKENS, H, head_dim)
    value_heads = values.astype(jnp.float32).reshape(TOKENS, H, head_dim)
    row_block = min(TOKENS, 128)
    block_count = TOKENS // row_block

    def one_block(block_index):
        first_row = (block_index * row_block).astype(jnp.int32)
        pair_rows = lax.dynamic_slice_in_dim(pair, first_row, row_block, 0).astype(jnp.float32)
        pair_normed = normalize(pair_rows).astype(jnp.bfloat16)
        pair_bias = jnp.einsum('ikc,ch->hik', pair_normed.astype(jnp.float32), pair_proj.astype(jnp.float32)).astype(jnp.bfloat16)
        query_rows = lax.dynamic_slice_in_dim(queries, first_row, row_block, 0).astype(jnp.float32)
        query_rows = query_rows.reshape(row_block, H, head_dim)
        scores = jnp.einsum('qhd,khd->hqk', query_rows, key_heads) * score_scale + pair_bias.astype(jnp.float32)
        scores = jnp.where(key_live[None, None, :], scores, -1e+30)
        maxima = lax.optimization_barrier(jnp.max(scores, axis=-1, keepdims=True))
        weights = jnp.exp(scores - maxima)
        totals = lax.optimization_barrier(jnp.sum(weights, axis=-1))
        rounded = weights.astype(jnp.bfloat16)
        numerator = jnp.einsum('hqk,khd->qhd', rounded.astype(jnp.float32), value_heads)
        return numerator / jnp.transpose(totals)[:, :, None]
    averaged = lax.map(one_block, jnp.arange(block_count, dtype=jnp.int32)).reshape(TOKENS, features)
    attended = (gating * averaged).astype(jnp.bfloat16)
    return jnp.dot(attended, out_proj, preferred_element_type=jnp.float32).astype(jnp.bfloat16)
```

```python
import functools

import jax
import jax.numpy as jnp
from jax import lax
from jax.experimental import pallas as pl
from jax.experimental.pallas import tpu as pltpu
from jax.sharding import PartitionSpec as P

LANES = 128
MASKED = -1e30
FLOOR = -1e28
F32 = jnp.float32
BF16 = jnp.bfloat16


def peer(axis, index):
    return dict(device_id={axis: index}, device_id_type=pl.DeviceIdType.MESH)


def normalize(rows, axis):
    centered = rows - jnp.mean(rows, axis=axis, keepdims=True)
    variance = jnp.mean(centered * centered, axis=axis, keepdims=True)
    return centered * lax.rsqrt(variance + 1e-05)


def matmul(a, b):
    return jnp.dot(a, b, preferred_element_type=F32)


def iota(shape, dim):
    return lax.broadcasted_iota(jnp.int32, shape, dim)


def flat(blocks):
    count, rows, width = blocks.shape
    return blocks.astype(F32).reshape(count * rows, width).astype(BF16)


def kernel(
    rows_n,
    cols_n,
    chunks,
    singles,
    pair,
    chain,
    proj,
    q_bias,
    pair_proj,
    out_proj,
    out,
    own_v,
    pair_v,
    chain_s,
    proj_v,
    q_bias_v,
    pair_proj_v,
    out_proj_v,
    query_in,
    row_in,
    key_in,
    bias_v,
    score_v,
    weight_v,
    value_v,
    part_out,
    part_in,
    load_sem,
    pair_sem,
    query_send,
    query_recv,
    row_send,
    row_recv,
    key_send,
    key_recv,
    part_send,
    part_recv,
):
    own, features = own_v.shape
    tile_rows, tile_cols, channels = pair_v.shape
    heads = pair_proj_v.shape[1]
    head_dim = features // heads
    lane_blocks = features // LANES
    slots = chain_s.shape[0]
    scale = head_dim ** (-0.5)
    row = lax.axis_index("rows")
    col = lax.axis_index("cols")

    loads = [
        pltpu.make_async_copy(src, dst, load_sem.at[n])
        for n, (src, dst) in enumerate(
            [
                (singles, own_v),
                (pair_proj, pair_proj_v),
                (proj, proj_v),
                (q_bias, q_bias_v),
                (out_proj, out_proj_v),
                (chain, chain_s),
            ]
        )
    ]
    step = tile_rows // chunks
    pieces = [
        pltpu.make_async_copy(
            pair.at[pl.ds(n * step, step)], pair_v.at[pl.ds(n * step, step)], pair_sem.at[n]
        )
        for n in range(chunks)
    ]
    loads[0].start()
    loads[1].start()
    pieces[0].start()
    for load in loads[2:]:
        load.start()
    for piece in pieces[1:]:
        piece.start()

    barrier = pltpu.get_barrier_semaphore()
    for d in range(1, cols_n):
        pl.semaphore_signal(barrier, inc=1, **peer("cols", lax.rem(col + d, cols_n)))
    for d in range(1, rows_n):
        pl.semaphore_signal(barrier, inc=1, **peer("rows", lax.rem(row + d, rows_n)))

    def far_first(count):
        return sorted(range(1, count), key=lambda d: -min(d, count - d))

    def send(src, dst, sems, axis, index, mine, target):
        return pltpu.make_async_remote_copy(
            src_ref=src,
            dst_ref=dst,
            send_sem=sems[0].at[target],
            recv_sem=sems[1].at[mine],
            **peer(axis, index),
        )

    def query_copy(other):
        return send(
            query_in.at[col], query_in.at[col], (query_send, query_recv), "cols", other, col, other
        )

    def row_copy(other):
        return send(row_in.at[row], row_in.at[row], (row_send, row_recv), "rows", other, row, other)

    def key_copy(other):
        return send(row_in.at[other], key_in.at[col], (key_send, key_recv), "cols", other, col, other)

    def part_copy(other):
        return send(
            part_out.at[other], part_in.at[col], (part_send, part_recv), "cols", other, col, other
        )

    def arrival(buf, sems, axis, index):
        return send(buf.at[index], buf.at[index], sems, axis, index, index, index)

    loads[0].wait()
    normed = normalize(own_v[...].astype(F32), -1).astype(BF16)
    query_in[pl.ds(col, 1)] = normed[None]
    row_in[pl.ds(row, 1)] = normed[None]

    loads[1].wait()
    pair_w = jnp.transpose(pair_proj_v[...].astype(F32)).astype(BF16)

    def tile_bias(first, last):
        @pl.loop(first, last, unroll=2)
        def _(i):
            block = jnp.transpose(pair_v[i]).astype(F32)
            block_normed = normalize(block, 0).astype(BF16)
            bias = matmul(pair_w, block_normed)
            bias_v[pl.ds(pl.multiple_of(i * heads, heads), heads), :] = bias.astype(BF16).astype(F32)

    def bias_chunks(first, last):
        for n in range(first, last):
            pieces[n].wait()
            tile_bias(n * step, (n + 1) * step)

    bias_chunks(0, chunks // 4)
    pl.semaphore_wait(barrier, cols_n + rows_n - 2)
    for d in far_first(rows_n):
        row_copy(lax.rem(row + d, rows_n)).start()
    for d in far_first(cols_n):
        query_copy(lax.rem(col + d, cols_n)).start()

    loads[2].wait()
    loads[3].wait()
    own_gate = jax.nn.sigmoid(matmul(normed, proj_v[:, 3 * features :]))
    bias_chunks(chunks // 4, chunks // 2)

    for d in range(1, rows_n):
        arrival(row_in, (row_send, row_recv), "rows", lax.rem(row + d, rows_n)).wait_recv()
    for d in far_first(cols_n):
        key_copy(lax.rem(col + d, cols_n)).start()
    key_in[pl.ds(col, 1)] = row_in[pl.ds(col, 1)]
    bias_chunks(chunks // 2, chunks)

    for d in range(1, cols_n):
        arrival(query_in, (query_send, query_recv), "cols", lax.rem(col + d, cols_n)).wait_recv()
    queries = (
        matmul(flat(query_in[...]), proj_v[:, :features]) + q_bias_v[...]
    ).astype(BF16).astype(F32)
    for d in range(1, cols_n):
        arrival(key_in, (key_send, key_recv), "cols", lax.rem(col + d, cols_n)).wait_recv()
    key_side = matmul(flat(key_in[...]), proj_v[:, features : 3 * features]).astype(BF16)
    keys = key_side[:, :features]
    values = key_side[:, features:].astype(F32)

    def heads_of(b):
        return [
            h
            for h in range(heads)
            if h * head_dim < (b + 1) * LANES and (h + 1) * head_dim > b * LANES
        ]

    def head_lanes(b, h):
        feature = iota((1, LANES), 1) + b * LANES
        return (feature >= h * head_dim) & (feature < (h + 1) * head_dim)

    seen = set()
    for b in range(lane_blocks):
        members = heads_of(b)
        block = slice(b * LANES, (b + 1) * LANES)
        stacked = jnp.concatenate(
            [jnp.where(head_lanes(b, h), queries[:, block], 0.0).astype(BF16) for h in members], axis=0
        )
        scores = lax.dot_general(
            stacked, keys[:, block], (((1,), (1,)), ((), ())), preferred_element_type=F32
        )
        for n, h in enumerate(members):
            part = scores[n * tile_rows : (n + 1) * tile_rows]
            score_v[h] = score_v[h] + part if h in seen else part
            seen.add(h)
            value_v[b, n * tile_cols : (n + 1) * tile_cols, :] = jnp.where(
                head_lanes(b, h), values[:, block], 0.0
            ).astype(BF16)

    loads[5].wait()
    live = chain_s[0]
    for n in range(1, slots - 1):
        live = live + chain_s[n]
    key_live = iota((1, tile_cols), 1) + col * tile_cols < live
    lane = iota((1, LANES), 1)
    top = jnp.zeros((tile_rows, LANES), F32)
    for h in range(heads):
        scores = score_v[h] * scale + bias_v[pl.ds(h, tile_rows, stride=heads), :]
        scores = jnp.where(key_live, scores, MASKED)
        largest = jnp.maximum(jnp.max(scores, axis=-1, keepdims=True), FLOOR)
        weight_v[:, h * tile_cols : (h + 1) * tile_cols] = jnp.exp(scores - largest).astype(BF16)
        top = jnp.where(lax.rem(lane, heads) == h, largest, top)

    ones_row = lax.div(iota((heads * tile_cols, LANES), 0), tile_cols)
    ones_lane = iota((heads * tile_cols, LANES), 1)
    ones = jnp.where(
        (lax.rem(ones_lane, heads) == ones_row) & (ones_lane < 2 * heads), 1.0, 0.0
    ).astype(BF16)
    stats = jnp.where(lane < 2 * heads, matmul(weight_v[...], ones), top)
    first = stats.astype(BF16).astype(F32)
    second = (stats - first).astype(BF16).astype(F32)
    third = stats - first - second
    group = lax.div(lane, heads)
    stats = jnp.where(
        (group == 0) | (group == 2), first, jnp.where((group == 1) | (group == 3), second, third)
    )
    stats = jnp.where(group < 5, stats, 0.0).astype(BF16)
    own_rows = tile_rows // cols_n
    part_out[:, :, features:] = stats.astype(F32).reshape(cols_n, own_rows, LANES).astype(BF16)
    for b in range(lane_blocks):
        members = heads_of(b)
        summed = matmul(
            weight_v[:, members[0] * tile_cols : (members[-1] + 1) * tile_cols],
            value_v[b, : len(members) * tile_cols, :],
        )
        part_out[:, :, b * LANES : (b + 1) * LANES] = summed.reshape(
            cols_n, own_rows, LANES
        ).astype(BF16)

    part_in[pl.ds(col, 1)] = part_out[pl.ds(col, 1)]
    for d in far_first(cols_n):
        part_copy(lax.rem(col + d, cols_n)).start()
    loads[4].wait()
    spread_row = iota((LANES, features), 0)
    spread_head = lax.div(iota((LANES, features), 1), head_dim)
    matches = lax.rem(spread_row, heads) == spread_head
    spread_group = lax.div(spread_row, heads)
    to_total = jnp.where(matches & (spread_group < 2), 1.0, 0.0).astype(BF16)
    to_top = jnp.where(matches & (spread_group >= 2) & (spread_group < 5), 1.0, 0.0).astype(BF16)
    for d in range(1, cols_n):
        arrival(part_in, (part_send, part_recv), "cols", lax.rem(col + d, cols_n)).wait_recv()
    arrived = flat(part_in[:, :, features:])
    total = matmul(arrived, to_total).reshape(cols_n, own_rows, features)
    tops = matmul(arrived, to_top).reshape(cols_n, own_rows, features)
    factor = jnp.exp(tops - jnp.max(tops, axis=0, keepdims=True))
    total = jnp.sum(factor * total, axis=0)
    numerator = jnp.sum(factor * part_in[:, :, :features].astype(F32), axis=0)
    attended = (own_gate * (numerator / total)).astype(BF16)
    out[...] = matmul(attended, out_proj_v[...]).astype(BF16)

    for d in range(1, rows_n):
        row_copy(lax.rem(row + d, rows_n)).wait_send()
    for d in range(1, cols_n):
        other = lax.rem(col + d, cols_n)
        query_copy(other).wait_send()
        key_copy(other).wait_send()
        part_copy(other).wait_send()


def shards(rows_n, cols_n, singles, pair, chain_sizes, single_proj, query_bias, pair_proj, out_proj):
    own, features = singles.shape
    tile_rows, tile_cols, channels = pair.shape
    heads = pair_proj.shape[1]
    chunks = 16
    dma = pltpu.SemaphoreType.DMA
    lane_blocks = features // LANES
    widest = -(-LANES // (features // heads)) + 1
    return pl.pallas_call(
        functools.partial(kernel, rows_n, cols_n, chunks),
        out_shape=jax.ShapeDtypeStruct((own, features), BF16),
        in_specs=[pl.BlockSpec(memory_space=pl.ANY)] * 7,
        out_specs=pl.BlockSpec(memory_space=pltpu.VMEM),
        scratch_shapes=[
            pltpu.VMEM((own, features), BF16),
            pltpu.VMEM(pair.shape, BF16),
            pltpu.SMEM(chain_sizes.shape, jnp.int32),
            pltpu.VMEM(single_proj.shape, BF16),
            pltpu.VMEM((1, features), F32),
            pltpu.VMEM(pair_proj.shape, BF16),
            pltpu.VMEM(out_proj.shape, BF16),
            pltpu.VMEM((cols_n, own, features), BF16),
            pltpu.VMEM((rows_n, own, features), BF16),
            pltpu.VMEM((cols_n, own, features), BF16),
            pltpu.VMEM((tile_rows * heads, tile_cols), F32),
            pltpu.VMEM((heads, tile_rows, tile_cols), F32),
            pltpu.VMEM((tile_rows, heads * tile_cols), BF16),
            pltpu.VMEM((lane_blocks, widest * tile_cols, LANES), BF16),
            pltpu.VMEM((cols_n, own, features + LANES), BF16),
            pltpu.VMEM((cols_n, own, features + LANES), BF16),
            dma((6,)),
            dma((chunks,)),
            dma((cols_n,)),
            dma((cols_n,)),
            dma((rows_n,)),
            dma((rows_n,)),
            dma((cols_n,)),
            dma((cols_n,)),
            dma((cols_n,)),
            dma((cols_n,)),
        ],
        compiler_params=pltpu.CompilerParams(collective_id=0, has_side_effects=True),
    )(singles, pair, chain_sizes, single_proj, query_bias.reshape(1, features), pair_proj, out_proj)


def solution(mesh):
    placed = (
        P(("parts", "rows", "cols"), None),
        P(("parts", "rows"), "cols", None),
        P("parts"),
        P(),
        P(),
        P(),
        P(),
    )
    return jax.shard_map(
        functools.partial(shards, mesh.shape["rows"], mesh.shape["cols"]),
        mesh=mesh,
        in_specs=placed,
        out_specs=P(("parts", "rows", "cols"), None),
        check_vma=False,
    )
```

```python
import functools

import jax
import jax.numpy as jnp
from jax import lax
from jax.experimental import pallas as pl
from jax.experimental.pallas import tpu as pltpu
from jax.sharding import PartitionSpec as P

LANES = 128
MASKED = -1e30
FLOOR = -1e28
F32 = jnp.float32
BF16 = jnp.bfloat16


def peer(axis, index):
    return dict(device_id={axis: index}, device_id_type=pl.DeviceIdType.MESH)


def normalize(rows, axis):
    centered = rows - jnp.mean(rows, axis=axis, keepdims=True)
    variance = jnp.mean(centered * centered, axis=axis, keepdims=True)
    return centered * lax.rsqrt(variance + 1e-05)


def matmul(a, b):
    return jnp.dot(a, b, preferred_element_type=F32)


def iota(shape, dim):
    return lax.broadcasted_iota(jnp.int32, shape, dim)


def flat(blocks):
    count, rows, width = blocks.shape
    return blocks.astype(F32).reshape(count * rows, width).astype(BF16)


def kernel(
    rows_n,
    cols_n,
    chunks,
    singles,
    pair,
    chain,
    proj,
    q_bias,
    pair_proj,
    out_proj,
    out,
    own_v,
    pair_v,
    chain_s,
    proj_v,
    q_bias_v,
    pair_proj_v,
    out_proj_v,
    query_in,
    row_in,
    key_in,
    bias_v,
    score_v,
    weight_v,
    value_v,
    part_out,
    part_in,
    load_sem,
    pair_sem,
    query_send,
    query_recv,
    row_send,
    row_recv,
    key_send,
    key_recv,
    up_in,
    up_send,
    up_recv,
    down_in,
    down_send,
    down_recv,
    twin_send,
    twin_recv,
    part_send,
    part_recv,
):
    own, features = own_v.shape
    tile_rows, tile_cols, channels = pair_v.shape
    heads = pair_proj_v.shape[0]
    head_dim = features // heads
    lane_blocks = features // LANES
    slots = chain_s.shape[0]
    scale = head_dim ** (-0.5)
    row = lax.axis_index("rows")
    col = lax.axis_index("cols")

    loads = [
        pltpu.make_async_copy(src, dst, load_sem.at[n])
        for n, (src, dst) in enumerate(
            [
                (singles, own_v),
                (pair_proj, pair_proj_v),
                (proj, proj_v),
                (q_bias, q_bias_v.at[0]),
                (out_proj, out_proj_v),
                (chain, chain_s),
            ]
        )
    ]
    step = tile_rows // chunks
    pieces = [
        pltpu.make_async_copy(
            pair.at[pl.ds(n * step, step)], pair_v.at[pl.ds(n * step, step)], pair_sem.at[n]
        )
        for n in range(chunks)
    ]
    loads[0].start()
    loads[1].start()
    pieces[0].start()
    for load in loads[2:]:
        load.start()
    for piece in pieces[1:]:
        piece.start()

    reach = cols_n // 4
    core = lax.rem(row, 2)
    chips = rows_n // 2
    near = [d for n in range(reach, 0, -1) for d in (n, -n)]

    def along(d):
        return lax.rem(col + d + cols_n, cols_n)

    def across(d):
        return lax.rem(row + 2 * d, rows_n)

    def mine(target):
        return lax.rem(target, 2) == core

    barrier = pltpu.get_barrier_semaphore()
    for d in near:
        pl.semaphore_signal(barrier, inc=1, **peer("cols", along(d)))
    for d in range(1, chips):
        pl.semaphore_signal(barrier, inc=1, **peer("rows", across(d)))
    twin = row + 1 - 2 * core
    pl.semaphore_signal(barrier, inc=1, **peer("rows", twin))

    def send(src, dst, sent, arrived, axis, index):
        return pltpu.make_async_remote_copy(
            src_ref=src, dst_ref=dst, send_sem=sent, recv_sem=arrived, **peer(axis, index)
        )

    def query_copy(slot, target, stage):
        return send(
            query_in.at[slot],
            query_in.at[slot],
            query_send.at[stage, target],
            query_recv.at[slot],
            "cols",
            target,
        )

    def row_copy(target):
        return send(
            row_in.at[row], row_in.at[row], row_send.at[target], row_recv.at[row], "rows", target
        )

    def key_copy(src, slot, target, stage):
        return send(
            src, key_in.at[slot], key_send.at[stage, target], key_recv.at[slot], "cols", target
        )

    def up_copy(n):
        return send(
            row_in.at[along(reach + 1 + n)],
            up_in.at[n],
            up_send.at[n],
            up_recv.at[n],
            "cols",
            along(reach),
        )

    def down_copy(n):
        return send(
            row_in.at[along(-reach - 1 - n)],
            down_in.at[n],
            down_send.at[n],
            down_recv.at[n],
            "cols",
            along(-reach),
        )

    def twin_copy():
        return send(key_in, key_in, twin_send, twin_recv, "rows", twin)

    def part_copy(other):
        return send(
            part_out.at[other],
            part_in.at[col],
            part_send.at[other],
            part_recv.at[col],
            "cols",
            other,
        )

    def query_stage(act):
        for d in near:
            act(query_copy(col, along(d), 0))

    def query_relay(direction, act):
        for n in range(reach if direction > 0 else reach - 1, 0, -1):
            act(query_copy(along(-direction * reach), along(direction * n), 1))

    def key_stage(act):
        for n in range(reach - 1, -1, -1):

            @pl.when(mine(along(reach + 1 + n)))
            def _():
                act(up_copy(n))

            if n < reach - 1:

                @pl.when(mine(along(-reach - 1 - n)))
                def _():
                    act(down_copy(n))

        for d in near:
            target = along(d)

            @pl.when(mine(target))
            def _():
                act(key_copy(row_in.at[target], col, target, 0))

    def key_relay(act, wait):
        for n in range(reach - 1, -1, -1):
            target = along(n + 1)

            @pl.when(mine(target))
            def _():
                if wait:
                    up_copy(n).wait_recv()
                act(key_copy(up_in.at[n], along(-reach), target, 1))

        for n in range(reach - 2, -1, -1):
            target = along(-n - 1)

            @pl.when(mine(target))
            def _():
                if wait:
                    down_copy(n).wait_recv()
                act(key_copy(down_in.at[n], along(reach), target, 1))

    def start(copy):
        copy.start()

    def wait_send(copy):
        copy.wait_send()

    far_first = sorted(range(1, cols_n), key=lambda d: -min(d, cols_n - d))

    loads[0].wait()
    normed = normalize(own_v[...].astype(F32), -1).astype(BF16)
    query_in[pl.ds(col, 1)] = normed[None]
    row_in[pl.ds(row, 1)] = normed[None]

    loads[1].wait()
    pair_w = pair_proj_v[...]

    def tile_bias(first, last):
        @pl.loop(first, last, unroll=4)
        def _(i):
            block = jnp.transpose(pair_v[i]).astype(F32)
            block_normed = normalize(block, 0).astype(BF16)
            bias = matmul(pair_w, block_normed)
            bias_v[pl.ds(pl.multiple_of(i * heads, heads), heads), :] = bias.astype(BF16).astype(F32)

    def bias_chunks(first, last):
        for n in range(first, last):
            pieces[n].wait()
            tile_bias(n * step, (n + 1) * step)

    bias_chunks(0, chunks // 4)
    pl.semaphore_wait(barrier, len(near) + chips)
    for d in range(1, chips):
        row_copy(across(d)).start()
    query_stage(start)
    bias_chunks(chunks // 4, 3 * chunks // 4)

    query_copy(along(-reach), along(-reach), 0).wait_recv()
    query_relay(1, start)
    query_copy(along(reach), along(reach), 0).wait_recv()
    query_relay(-1, start)
    for d in range(1, chips):
        send(
            row_in.at[across(d)],
            row_in.at[across(d)],
            row_send.at[across(d)],
            row_recv.at[across(d)],
            "rows",
            across(d),
        ).wait_recv()
    key_stage(start)

    @pl.when(mine(col))
    def _():
        key_in[pl.ds(col, 1)] = row_in[pl.ds(col, 1)]

    loads[2].wait()
    loads[3].wait()
    own_gate = jax.nn.sigmoid(matmul(normed, proj_v[:, 3 * features :]))
    bias_chunks(3 * chunks // 4, chunks)
    key_relay(start, True)

    for d in far_first:
        if d not in (reach, cols_n - reach):
            query_copy(along(d), along(d), 0).wait_recv()
    queries = (
        matmul(flat(query_in[...]), proj_v[:, :features]) + q_bias_v[...]
    ).astype(BF16).astype(F32)

    @pl.when(mine(col))
    def _():
        for d in far_first:
            key_copy(key_in.at[along(d)], along(d), along(d), 0).wait_recv()
        twin_copy().start()

    @pl.when(jnp.logical_not(mine(col)))
    def _():
        twin_copy().wait_recv()

    key_side = matmul(flat(key_in[...]), proj_v[:, features : 3 * features]).astype(BF16)
    keys = key_side[:, :features]
    values = key_side[:, features:].astype(F32)

    def heads_of(b):
        return [
            h
            for h in range(heads)
            if h * head_dim < (b + 1) * LANES and (h + 1) * head_dim > b * LANES
        ]

    def head_lanes(b, h):
        feature = iota((1, LANES), 1) + b * LANES
        return (feature >= h * head_dim) & (feature < (h + 1) * head_dim)

    seen = set()
    for b in range(lane_blocks):
        members = heads_of(b)
        block = slice(b * LANES, (b + 1) * LANES)
        stacked = jnp.concatenate(
            [jnp.where(head_lanes(b, h), queries[:, block], 0.0).astype(BF16) for h in members], axis=0
        )
        scores = lax.dot_general(
            stacked, keys[:, block], (((1,), (1,)), ((), ())), preferred_element_type=F32
        )
        for n, h in enumerate(members):
            part = scores[n * tile_rows : (n + 1) * tile_rows]
            score_v[h] = score_v[h] + part if h in seen else part
            seen.add(h)
            value_v[b, n * tile_cols : (n + 1) * tile_cols, :] = jnp.where(
                head_lanes(b, h), values[:, block], 0.0
            ).astype(BF16)

    loads[5].wait()
    live = chain_s[0]
    for n in range(1, slots - 1):
        live = live + chain_s[n]
    key_live = iota((1, tile_cols), 1) + col * tile_cols < live
    lane = iota((1, LANES), 1)
    top = jnp.zeros((tile_rows, LANES), F32)
    for h in range(heads):
        scores = score_v[h] * scale + bias_v[pl.ds(h, tile_rows, stride=heads), :]
        scores = jnp.where(key_live, scores, MASKED)
        largest = jnp.maximum(jnp.max(scores, axis=-1, keepdims=True), FLOOR)
        weight_v[:, h * tile_cols : (h + 1) * tile_cols] = jnp.exp(scores - largest).astype(BF16)
        top = jnp.where(lax.rem(lane, heads) == h, largest, top)

    ones_row = lax.div(iota((heads * tile_cols, LANES), 0), tile_cols)
    ones_lane = iota((heads * tile_cols, LANES), 1)
    ones = jnp.where(
        (lax.rem(ones_lane, heads) == ones_row) & (ones_lane < 2 * heads), 1.0, 0.0
    ).astype(BF16)
    stats = jnp.where(lane < 2 * heads, matmul(weight_v[...], ones), top)
    first = stats.astype(BF16).astype(F32)
    second = (stats - first).astype(BF16).astype(F32)
    third = stats - first - second
    group = lax.div(lane, heads)
    stats = jnp.where(
        (group == 0) | (group == 2), first, jnp.where((group == 1) | (group == 3), second, third)
    )
    stats = jnp.where(group < 5, stats, 0.0).astype(BF16)
    own_rows = tile_rows // cols_n
    part_out[:, :, features:] = stats.astype(F32).reshape(cols_n, own_rows, LANES).astype(BF16)
    for b in range(lane_blocks):
        members = heads_of(b)
        summed = matmul(
            weight_v[:, members[0] * tile_cols : (members[-1] + 1) * tile_cols],
            value_v[b, : len(members) * tile_cols, :],
        )
        part_out[:, :, b * LANES : (b + 1) * LANES] = summed.reshape(
            cols_n, own_rows, LANES
        ).astype(BF16)

    part_in[pl.ds(col, 1)] = part_out[pl.ds(col, 1)]
    for d in far_first:
        part_copy(along(d)).start()
    loads[4].wait()
    spread_row = iota((LANES, features), 0)
    spread_head = lax.div(iota((LANES, features), 1), head_dim)
    matches = lax.rem(spread_row, heads) == spread_head
    spread_group = lax.div(spread_row, heads)
    to_total = jnp.where(matches & (spread_group < 2), 1.0, 0.0).astype(BF16)
    to_top = jnp.where(matches & (spread_group >= 2) & (spread_group < 5), 1.0, 0.0).astype(BF16)
    for d in far_first:
        send(
            part_in.at[along(d)],
            part_in.at[along(d)],
            part_send.at[along(d)],
            part_recv.at[along(d)],
            "cols",
            along(d),
        ).wait_recv()
    arrived = flat(part_in[:, :, features:])
    total = matmul(arrived, to_total).reshape(cols_n, own_rows, features)
    tops = matmul(arrived, to_top).reshape(cols_n, own_rows, features)
    factor = jnp.exp(tops - jnp.max(tops, axis=0, keepdims=True))
    total = jnp.sum(factor * total, axis=0)
    numerator = jnp.sum(factor * part_in[:, :, :features].astype(F32), axis=0)
    attended = (own_gate * (numerator / total)).astype(BF16)
    out[...] = matmul(attended, out_proj_v[...]).astype(BF16)

    for d in range(1, chips):
        row_copy(across(d)).wait_send()
    query_stage(wait_send)
    query_relay(1, wait_send)
    query_relay(-1, wait_send)
    key_stage(wait_send)
    key_relay(wait_send, False)

    @pl.when(mine(col))
    def _():
        twin_copy().wait_send()

    for d in far_first:
        part_copy(along(d)).wait_send()


def shards(rows_n, cols_n, singles, pair, chain_sizes, single_proj, query_bias, pair_proj, out_proj):
    own, features = singles.shape
    tile_rows, tile_cols, channels = pair.shape
    heads = pair_proj.shape[1]
    chunks = 8
    reach = cols_n // 4
    dma = pltpu.SemaphoreType.DMA
    lane_blocks = features // LANES
    widest = -(-LANES // (features // heads)) + 1
    return pl.pallas_call(
        functools.partial(kernel, rows_n, cols_n, chunks),
        out_shape=pltpu.VMEM((own, features), BF16),
        in_specs=[pl.BlockSpec(memory_space=pl.ANY)] * 7,
        out_specs=pl.BlockSpec(memory_space=pltpu.VMEM),
        scratch_shapes=[
            pltpu.VMEM((own, features), BF16),
            pltpu.VMEM(pair.shape, BF16),
            pltpu.SMEM(chain_sizes.shape, jnp.int32),
            pltpu.VMEM(single_proj.shape, BF16),
            pltpu.VMEM((1, features), F32),
            pltpu.VMEM((heads, channels), BF16),
            pltpu.VMEM(out_proj.shape, BF16),
            pltpu.VMEM((cols_n, own, features), BF16),
            pltpu.VMEM((rows_n, own, features), BF16),
            pltpu.VMEM((cols_n, own, features), BF16),
            pltpu.VMEM((tile_rows * heads, tile_cols), F32),
            pltpu.VMEM((heads, tile_rows, tile_cols), F32),
            pltpu.VMEM((tile_rows, heads * tile_cols), BF16),
            pltpu.VMEM((lane_blocks, widest * tile_cols, LANES), BF16),
            pltpu.VMEM((cols_n, own, features + LANES), BF16),
            pltpu.VMEM((cols_n, own, features + LANES), BF16),
            dma((6,)),
            dma((chunks,)),
            dma((2, cols_n)),
            dma((cols_n,)),
            dma((rows_n,)),
            dma((rows_n,)),
            dma((2, cols_n)),
            dma((cols_n,)),
            pltpu.VMEM((reach, own, features), BF16),
            dma((reach,)),
            dma((reach,)),
            pltpu.VMEM((reach, own, features), BF16),
            dma((reach,)),
            dma((reach,)),
            dma,
            dma,
            dma((cols_n,)),
            dma((cols_n,)),
        ],
        compiler_params=pltpu.CompilerParams(collective_id=0, has_side_effects=True),
    )(singles, pair, chain_sizes, single_proj, query_bias, pair_proj.T, out_proj)


def solution(mesh):
    placed = (
        P(("parts", "rows", "cols"), None),
        P(("parts", "rows"), "cols", None),
        P("parts"),
        P(),
        P(),
        P(),
        P(),
    )
    return jax.shard_map(
        functools.partial(shards, mesh.shape["rows"], mesh.shape["cols"]),
        mesh=mesh,
        in_specs=placed,
        out_specs=P(("parts", "rows", "cols"), None),
        check_vma=False,
    )
```

```python
import functools

import jax
import jax.numpy as jnp
from jax import lax
from jax.experimental import pallas as pl
from jax.experimental.pallas import tpu as pltpu
from jax.sharding import PartitionSpec as P

LANES = 128
MASKED = -1e30
FLOOR = -1e28
F32 = jnp.float32
BF16 = jnp.bfloat16


def peer(**place):
    return dict(device_id=place, device_id_type=pl.DeviceIdType.MESH)


def normalize(rows, axis):
    centered = rows - jnp.mean(rows, axis=axis, keepdims=True)
    variance = jnp.mean(centered * centered, axis=axis, keepdims=True)
    return centered * lax.rsqrt(variance + 1e-05)


def matmul(a, b):
    return jnp.dot(a, b, preferred_element_type=F32)


def iota(shape, dim):
    return lax.broadcasted_iota(jnp.int32, shape, dim)


def flat(blocks):
    count, rows, width = blocks.shape
    return blocks.astype(F32).reshape(count * rows, width).astype(BF16)


def kernel(
    rows_n,
    cols_n,
    chunks,
    singles,
    pair,
    chain,
    proj,
    q_bias,
    pair_proj,
    out_proj,
    out,
    own_v,
    pair_v,
    chain_s,
    proj_v,
    q_bias_v,
    pair_proj_v,
    out_proj_v,
    query_in,
    key_in,
    bias_v,
    score_v,
    weight_v,
    value_v,
    part_out,
    part_in,
    load_sem,
    pair_sem,
    query_send,
    query_recv,
    key_send,
    key_recv,
    up_in,
    up_recv,
    down_in,
    down_recv,
    relay_send,
    part_send,
    part_recv,
):
    own, features = own_v.shape
    tile_rows, tile_cols, channels = pair_v.shape
    heads = pair_proj_v.shape[0]
    head_dim = features // heads
    lane_blocks = features // LANES
    slots = chain_s.shape[0]
    scale = head_dim ** (-0.5)
    row = lax.axis_index("rows")
    col = lax.axis_index("cols")

    loads = [
        pltpu.make_async_copy(src, dst, load_sem.at[n])
        for n, (src, dst) in enumerate(
            [
                (singles, own_v),
                (pair_proj, pair_proj_v),
                (proj, proj_v),
                (q_bias, q_bias_v.at[0]),
                (out_proj, out_proj_v),
                (chain, chain_s),
            ]
        )
    ]
    step = tile_rows // chunks
    pieces = [
        pltpu.make_async_copy(
            pair.at[pl.ds(n * step, step)], pair_v.at[pl.ds(n * step, step)], pair_sem.at[n]
        )
        for n in range(chunks)
    ]
    loads[0].start()
    loads[1].start()
    pieces[0].start()
    for load in loads[2:]:
        load.start()
    for piece in pieces[1:]:
        piece.start()

    reach = cols_n // 4
    near = [d for n in range(reach, 0, -1) for d in (n, -n)]

    def along(d):
        return lax.rem(col + d + cols_n, cols_n)

    offset = lax.rem(row - col + cols_n, cols_n)
    diagonal = offset == 0
    direct = (offset <= reach) | (offset >= cols_n - reach)
    upward = (offset > reach) & (offset <= 2 * reach)
    downward = (offset > 2 * reach) & (offset < cols_n - reach)

    barrier = pltpu.get_barrier_semaphore()

    def announce(**place):
        pl.semaphore_signal(barrier, inc=1, **peer(**place))

    for d in near:
        announce(cols=along(d))
        announce(rows=col, cols=along(d))
    for n in range(reach):
        announce(rows=along(n + 1), cols=along(-reach))
        if n < reach - 1:
            announce(rows=along(-n - 1), cols=along(reach))

    @pl.when(jnp.logical_not(diagonal))
    def _():
        announce(rows=col)

    def send(src, dst, sent, arrived, **place):
        return pltpu.make_async_remote_copy(
            src_ref=src, dst_ref=dst, send_sem=sent, recv_sem=arrived, **peer(**place)
        )

    def query_copy(slot, target, stage):
        return send(
            query_in.at[slot],
            query_in.at[slot],
            query_send.at[stage, target],
            query_recv.at[slot],
            cols=target,
        )

    def key_copy(target):
        return send(
            query_in.at[col],
            key_in.at[col],
            key_send.at[target],
            key_recv.at[col],
            rows=target,
            cols=row,
        )

    def up_copy(target):
        n = offset - reach - 1
        return send(
            query_in.at[col],
            up_in.at[n],
            key_send.at[target],
            up_recv.at[n],
            rows=target,
            cols=along(reach),
        )

    def down_copy(target):
        n = cols_n - offset - reach - 1
        return send(
            query_in.at[col],
            down_in.at[n],
            key_send.at[target],
            down_recv.at[n],
            rows=target,
            cols=along(-reach),
        )

    def relay_copy(src, slot, target):
        return send(src, key_in.at[slot], relay_send.at[target], key_recv.at[slot], cols=target)

    def landed(buf, sem, n):
        send(buf.at[n], buf.at[n], relay_send.at[0], sem.at[n], cols=along(1)).wait_recv()

    def part_copy(other):
        return send(
            part_out.at[other],
            part_in.at[col],
            part_send.at[other],
            part_recv.at[col],
            cols=other,
        )

    def query_stage(act):
        for d in near:
            act(query_copy(col, along(d), 0))

    def query_relay(direction, act):
        for n in range(reach if direction > 0 else reach - 1, 0, -1):
            act(query_copy(along(-direction * reach), along(direction * n), 1))

    def key_stage(act):
        @pl.when(direct)
        def _():
            for d in rows_far_first:
                act(key_copy(lax.rem(row + d, rows_n)))

            @pl.when(jnp.logical_not(diagonal))
            def _():
                act(key_copy(row))

        @pl.when(upward)
        def _():
            for d in rows_far_first + [0]:
                act(up_copy(lax.rem(row + d, rows_n)))

        @pl.when(downward)
        def _():
            for d in rows_far_first + [0]:
                act(down_copy(lax.rem(row + d, rows_n)))

    def key_relay(act, wait):
        for n in range(reach - 1, -1, -1):
            if wait:
                landed(up_in, up_recv, n)
            act(relay_copy(up_in.at[n], along(-reach), along(n + 1)))
        for n in range(reach - 2, -1, -1):
            if wait:
                landed(down_in, down_recv, n)
            act(relay_copy(down_in.at[n], along(reach), along(-n - 1)))

    def start(copy):
        copy.start()

    def wait_send(copy):
        copy.wait_send()

    rows_far_first = sorted(range(1, rows_n), key=lambda d: -min(d, rows_n - d))
    far_first = sorted(range(1, cols_n), key=lambda d: -min(d, cols_n - d))

    loads[0].wait()
    normed = normalize(own_v[...].astype(F32), -1).astype(BF16)
    query_in[pl.ds(col, 1)] = normed[None]

    @pl.when(diagonal)
    def _():
        key_in[pl.ds(col, 1)] = normed[None]


    loads[1].wait()
    pair_w = pair_proj_v[...]

    def tile_bias(first, last):
        @pl.loop(first, last, unroll=4)
        def _(i):
            block = jnp.transpose(pair_v[i]).astype(F32)
            block_normed = normalize(block, 0).astype(BF16)
            bias = matmul(pair_w, block_normed)
            bias_v[pl.ds(pl.multiple_of(i * heads, heads), heads), :] = bias.astype(BF16).astype(F32)

    def bias_chunks(first, last):
        for n in range(first, last):
            pieces[n].wait()
            tile_bias(n * step, (n + 1) * step)

    own_self = jnp.where(diagonal, 1, 0)
    pl.semaphore_wait(barrier, len(near) + cols_n - own_self)
    key_stage(start)
    query_stage(start)
    bias_chunks(0, chunks // 2)

    landed(query_in, query_recv, along(-reach))
    query_relay(1, start)
    landed(query_in, query_recv, along(reach))
    query_relay(-1, start)
    loads[2].wait()
    loads[3].wait()
    own_gate = jax.nn.sigmoid(matmul(normed, proj_v[:, 3 * features :]))
    bias_chunks(chunks // 2, 3 * chunks // 4)
    key_relay(start, True)
    bias_chunks(3 * chunks // 4, chunks)

    for d in far_first:
        if d not in (reach, cols_n - reach):
            landed(query_in, query_recv, along(d))
    queries = (
        matmul(flat(query_in[...]), proj_v[:, :features]) + q_bias_v[...]
    ).astype(BF16).astype(F32)

    for d in far_first:
        landed(key_in, key_recv, along(d))

    @pl.when(jnp.logical_not(diagonal))
    def _():
        landed(key_in, key_recv, col)

    key_side = matmul(flat(key_in[...]), proj_v[:, features : 3 * features]).astype(BF16)
    keys = key_side[:, :features]
    values = key_side[:, features:].astype(F32)

    def heads_of(b):
        return [
            h
            for h in range(heads)
            if h * head_dim < (b + 1) * LANES and (h + 1) * head_dim > b * LANES
        ]

    def head_lanes(b, h):
        feature = iota((1, LANES), 1) + b * LANES
        return (feature >= h * head_dim) & (feature < (h + 1) * head_dim)

    seen = set()
    for b in range(lane_blocks):
        members = heads_of(b)
        block = slice(b * LANES, (b + 1) * LANES)
        stacked = jnp.concatenate(
            [jnp.where(head_lanes(b, h), queries[:, block], 0.0).astype(BF16) for h in members], axis=0
        )
        scores = lax.dot_general(
            stacked, keys[:, block], (((1,), (1,)), ((), ())), preferred_element_type=F32
        )
        for n, h in enumerate(members):
            part = scores[n * tile_rows : (n + 1) * tile_rows]
            score_v[h] = score_v[h] + part if h in seen else part
            seen.add(h)
            value_v[b, n * tile_cols : (n + 1) * tile_cols, :] = jnp.where(
                head_lanes(b, h), values[:, block], 0.0
            ).astype(BF16)

    loads[5].wait()
    live = chain_s[0]
    for n in range(1, slots - 1):
        live = live + chain_s[n]
    key_live = iota((1, tile_cols), 1) + col * tile_cols < live
    lane = iota((1, LANES), 1)
    top = jnp.zeros((tile_rows, LANES), F32)
    for h in range(heads):
        scores = score_v[h] * scale + bias_v[pl.ds(h, tile_rows, stride=heads), :]
        scores = jnp.where(key_live, scores, MASKED)
        largest = jnp.maximum(jnp.max(scores, axis=-1, keepdims=True), FLOOR)
        weight_v[:, h * tile_cols : (h + 1) * tile_cols] = jnp.exp(scores - largest).astype(BF16)
        top = jnp.where(lax.rem(lane, heads) == h, largest, top)

    ones_row = lax.div(iota((heads * tile_cols, LANES), 0), tile_cols)
    ones_lane = iota((heads * tile_cols, LANES), 1)
    ones = jnp.where(
        (lax.rem(ones_lane, heads) == ones_row) & (ones_lane < 2 * heads), 1.0, 0.0
    ).astype(BF16)
    stats = jnp.where(lane < 2 * heads, matmul(weight_v[...], ones), top)
    first = stats.astype(BF16).astype(F32)
    second = (stats - first).astype(BF16).astype(F32)
    third = stats - first - second
    group = lax.div(lane, heads)
    stats = jnp.where(
        (group == 0) | (group == 2), first, jnp.where((group == 1) | (group == 3), second, third)
    )
    stats = jnp.where(group < 5, stats, 0.0).astype(BF16)
    own_rows = tile_rows // cols_n
    part_out[:, :, features:] = stats.astype(F32).reshape(cols_n, own_rows, LANES).astype(BF16)
    for b in range(lane_blocks):
        members = heads_of(b)
        summed = matmul(
            weight_v[:, members[0] * tile_cols : (members[-1] + 1) * tile_cols],
            value_v[b, : len(members) * tile_cols, :],
        )
        part_out[:, :, b * LANES : (b + 1) * LANES] = summed.reshape(
            cols_n, own_rows, LANES
        ).astype(BF16)

    part_in[pl.ds(col, 1)] = part_out[pl.ds(col, 1)]
    for d in far_first:
        part_copy(along(d)).start()
    loads[4].wait()
    spread_row = iota((LANES, features), 0)
    spread_head = lax.div(iota((LANES, features), 1), head_dim)
    matches = lax.rem(spread_row, heads) == spread_head
    spread_group = lax.div(spread_row, heads)
    to_total = jnp.where(matches & (spread_group < 2), 1.0, 0.0).astype(BF16)
    to_top = jnp.where(matches & (spread_group >= 2) & (spread_group < 5), 1.0, 0.0).astype(BF16)
    for d in far_first:
        landed(part_in, part_recv, along(d))
    arrived = flat(part_in[:, :, features:])
    total = matmul(arrived, to_total).reshape(cols_n, own_rows, features)
    tops = matmul(arrived, to_top).reshape(cols_n, own_rows, features)
    factor = jnp.exp(tops - jnp.max(tops, axis=0, keepdims=True))
    total = jnp.sum(factor * total, axis=0)
    numerator = jnp.sum(factor * part_in[:, :, :features].astype(F32), axis=0)
    attended = (own_gate * (numerator / total)).astype(BF16)
    out[...] = matmul(attended, out_proj_v[...]).astype(BF16)

    query_stage(wait_send)
    query_relay(1, wait_send)
    query_relay(-1, wait_send)
    key_stage(wait_send)
    key_relay(wait_send, False)

    for d in far_first:
        part_copy(along(d)).wait_send()


def shards(rows_n, cols_n, singles, pair, chain_sizes, single_proj, query_bias, pair_proj, out_proj):
    own, features = singles.shape
    tile_rows, tile_cols, channels = pair.shape
    heads = pair_proj.shape[1]
    chunks = 8
    reach = cols_n // 4
    dma = pltpu.SemaphoreType.DMA
    lane_blocks = features // LANES
    widest = -(-LANES // (features // heads)) + 1
    return pl.pallas_call(
        functools.partial(kernel, rows_n, cols_n, chunks),
        out_shape=pltpu.VMEM((own, features), BF16),
        in_specs=[pl.BlockSpec(memory_space=pl.ANY)] * 7,
        out_specs=pl.BlockSpec(memory_space=pltpu.VMEM),
        scratch_shapes=[
            pltpu.VMEM((own, features), BF16),
            pltpu.VMEM(pair.shape, BF16),
            pltpu.SMEM(chain_sizes.shape, jnp.int32),
            pltpu.VMEM(single_proj.shape, BF16),
            pltpu.VMEM((1, features), F32),
            pltpu.VMEM((heads, channels), BF16),
            pltpu.VMEM(out_proj.shape, BF16),
            pltpu.VMEM((cols_n, own, features), BF16),
            pltpu.VMEM((cols_n, own, features), BF16),
            pltpu.VMEM((tile_rows * heads, tile_cols), F32),
            pltpu.VMEM((heads, tile_rows, tile_cols), F32),
            pltpu.VMEM((tile_rows, heads * tile_cols), BF16),
            pltpu.VMEM((lane_blocks, widest * tile_cols, LANES), BF16),
            pltpu.VMEM((cols_n, own, features + LANES), BF16),
            pltpu.VMEM((cols_n, own, features + LANES), BF16),
            dma((6,)),
            dma((chunks,)),
            dma((2, cols_n)),
            dma((cols_n,)),
            dma((rows_n,)),
            dma((cols_n,)),
            pltpu.VMEM((reach, own, features), BF16),
            dma((reach,)),
            pltpu.VMEM((reach, own, features), BF16),
            dma((reach,)),
            dma((cols_n,)),
            dma((cols_n,)),
            dma((cols_n,)),
        ],
        compiler_params=pltpu.CompilerParams(collective_id=0, has_side_effects=True),
    )(singles, pair, chain_sizes, single_proj, query_bias, pair_proj.T, out_proj)


def solution(mesh):
    placed = (
        P(("parts", "rows", "cols"), None),
        P(("parts", "rows"), "cols", None),
        P("parts"),
        P(),
        P(),
        P(),
        P(),
    )
    return jax.shard_map(
        functools.partial(shards, mesh.shape["rows"], mesh.shape["cols"]),
        mesh=mesh,
        in_specs=placed,
        out_specs=P(("parts", "rows", "cols"), None),
        check_vma=False,
    )
```

```python
import functools

import jax
import jax.numpy as jnp
from jax import lax
from jax.experimental import pallas as pl
from jax.experimental.pallas import tpu as pltpu
from jax.sharding import PartitionSpec as P

LANES = 128
MASKED = -1e30
FLOOR = -1e28
F32 = jnp.float32
BF16 = jnp.bfloat16


def peer(**place):
    return dict(device_id=place, device_id_type=pl.DeviceIdType.MESH)


def normalize(rows, axis):
    centered = rows - jnp.mean(rows, axis=axis, keepdims=True)
    variance = jnp.mean(centered * centered, axis=axis, keepdims=True)
    return centered * lax.rsqrt(variance + 1e-05)


def matmul(a, b):
    return jnp.dot(a, b, preferred_element_type=F32)


def halves(distance):
    if distance in (0, 1):
        return distance + 1, -1
    if distance == -1:
        return -2, 1
    first = -(-abs(distance) // 2)
    sign = 1 if distance > 0 else -1
    return sign * first, distance - sign * first


def iota(shape, dim):
    return lax.broadcasted_iota(jnp.int32, shape, dim)


def flat(blocks):
    count, rows, width = blocks.shape
    return blocks.astype(F32).reshape(count * rows, width).astype(BF16)


def kernel(
    rows_n,
    cols_n,
    chunks,
    singles,
    pair,
    chain,
    proj,
    q_bias,
    pair_proj,
    out_proj,
    out,
    own_v,
    pair_v,
    chain_s,
    proj_v,
    q_bias_v,
    pair_proj_v,
    out_proj_v,
    query_in,
    key_in,
    bias_v,
    score_v,
    weight_v,
    value_v,
    part_out,
    part_in,
    load_sem,
    pair_sem,
    query_send,
    query_recv,
    key_send,
    key_recv,
    mid_in,
    mid_recv,
    relay_send,
    part_send,
    part_recv,
):
    own, features = own_v.shape
    tile_rows, tile_cols, channels = pair_v.shape
    heads = pair_proj_v.shape[0]
    head_dim = features // heads
    lane_blocks = features // LANES
    slots = chain_s.shape[0]
    scale = head_dim ** (-0.5)
    row = lax.axis_index("rows")
    col = lax.axis_index("cols")

    loads = [
        pltpu.make_async_copy(src, dst, load_sem.at[n])
        for n, (src, dst) in enumerate(
            [
                (singles, own_v),
                (pair_proj, pair_proj_v),
                (proj, proj_v),
                (q_bias, q_bias_v.at[0]),
                (out_proj, out_proj_v),
                (chain, chain_s),
            ]
        )
    ]
    step = tile_rows // chunks
    pieces = [
        pltpu.make_async_copy(
            pair.at[pl.ds(n * step, step)], pair_v.at[pl.ds(n * step, step)], pair_sem.at[n]
        )
        for n in range(chunks)
    ]
    loads[0].start()
    loads[1].start()
    pieces[0].start()
    for load in loads[2:]:
        load.start()
    for piece in pieces[1:]:
        piece.start()

    reach = cols_n // 4
    near = [d for n in range(reach, 0, -1) for d in (n, -n)]

    def along(d):
        return lax.rem(col + d + cols_n, cols_n)

    offset = lax.rem(row - col + cols_n, cols_n)
    splits = [(d % cols_n, *halves(d)) for d in range(cols_n // 2, -cols_n // 2, -1)]
    splits.sort(key=lambda split: -abs(split[2]))
    hop = 0
    for slot, first, second in splits:
        hop = hop + jnp.where(offset == slot, first, 0)

    barrier = pltpu.get_barrier_semaphore()

    def announce(**place):
        pl.semaphore_signal(barrier, inc=1, **peer(**place))

    for d in near:
        announce(cols=along(d))
    for slot, first, second in splits:
        announce(rows=along(second), cols=along(-first))

    def send(src, dst, sent, arrived, **place):
        return pltpu.make_async_remote_copy(
            src_ref=src, dst_ref=dst, send_sem=sent, recv_sem=arrived, **peer(**place)
        )

    def query_copy(slot, target, stage):
        return send(
            query_in.at[slot],
            query_in.at[slot],
            query_send.at[stage, target],
            query_recv.at[slot],
            cols=target,
        )

    def key_copy(target):
        return send(
            query_in.at[col],
            mid_in.at[offset],
            key_send.at[target],
            mid_recv.at[offset],
            rows=target,
            cols=along(hop),
        )

    def relay_copy(slot, first, second):
        return send(
            mid_in.at[slot],
            key_in.at[along(-first)],
            relay_send.at[slot],
            key_recv.at[along(-first)],
            cols=along(second),
        )

    def landed(buf, sem, n):
        send(buf.at[n], buf.at[n], relay_send.at[0], sem.at[n], cols=along(1)).wait_recv()

    def part_copy(other):
        return send(
            part_out.at[other],
            part_in.at[col],
            part_send.at[other],
            part_recv.at[col],
            cols=other,
        )

    def query_stage(act):
        for d in near:
            act(query_copy(col, along(d), 0))

    def query_relay(direction, act):
        for n in range(reach if direction > 0 else reach - 1, 0, -1):
            act(query_copy(along(-direction * reach), along(direction * n), 1))

    def key_stage(act):
        for d in rows_far_first + [0]:
            act(key_copy(lax.rem(row + d, rows_n)))

    def key_relay(act, wait):
        for slot, first, second in splits:
            if wait:
                landed(mid_in, mid_recv, slot)
            act(relay_copy(slot, first, second))

    def start(copy):
        copy.start()

    def wait_send(copy):
        copy.wait_send()

    rows_far_first = sorted(range(1, rows_n), key=lambda d: -min(d, rows_n - d))
    far_first = sorted(range(1, cols_n), key=lambda d: -min(d, cols_n - d))

    loads[0].wait()
    normed = normalize(own_v[...].astype(F32), -1).astype(BF16)
    query_in[pl.ds(col, 1)] = normed[None]

    loads[1].wait()
    pair_w = pair_proj_v[...]

    def tile_bias(first, last):
        @pl.loop(first, last, unroll=4)
        def _(i):
            block = jnp.transpose(pair_v[i]).astype(F32)
            block_normed = normalize(block, 0).astype(BF16)
            bias = matmul(pair_w, block_normed)
            bias_v[pl.ds(pl.multiple_of(i * heads, heads), heads), :] = bias.astype(BF16).astype(F32)

    def bias_chunks(first, last):
        for n in range(first, last):
            pieces[n].wait()
            tile_bias(n * step, (n + 1) * step)

    pl.semaphore_wait(barrier, len(near) + len(splits))
    key_stage(start)
    query_stage(start)
    bias_chunks(0, chunks // 2)

    landed(query_in, query_recv, along(-reach))
    query_relay(1, start)
    landed(query_in, query_recv, along(reach))
    query_relay(-1, start)
    loads[2].wait()
    loads[3].wait()
    own_gate = jax.nn.sigmoid(matmul(normed, proj_v[:, 3 * features :]))
    bias_chunks(chunks // 2, 3 * chunks // 4)
    key_relay(start, True)
    bias_chunks(3 * chunks // 4, chunks)

    for d in far_first:
        if d not in (reach, cols_n - reach):
            landed(query_in, query_recv, along(d))
    queries = (
        matmul(flat(query_in[...]), proj_v[:, :features]) + q_bias_v[...]
    ).astype(BF16).astype(F32)

    for d in far_first + [0]:
        landed(key_in, key_recv, along(d))

    key_side = matmul(flat(key_in[...]), proj_v[:, features : 3 * features]).astype(BF16)
    keys = key_side[:, :features]
    values = key_side[:, features:].astype(F32)

    def heads_of(b):
        return [
            h
            for h in range(heads)
            if h * head_dim < (b + 1) * LANES and (h + 1) * head_dim > b * LANES
        ]

    def head_lanes(b, h):
        feature = iota((1, LANES), 1) + b * LANES
        return (feature >= h * head_dim) & (feature < (h + 1) * head_dim)

    seen = set()
    for b in range(lane_blocks):
        members = heads_of(b)
        block = slice(b * LANES, (b + 1) * LANES)
        stacked = jnp.concatenate(
            [jnp.where(head_lanes(b, h), queries[:, block], 0.0).astype(BF16) for h in members], axis=0
        )
        scores = lax.dot_general(
            stacked, keys[:, block], (((1,), (1,)), ((), ())), preferred_element_type=F32
        )
        for n, h in enumerate(members):
            part = scores[n * tile_rows : (n + 1) * tile_rows]
            score_v[h] = score_v[h] + part if h in seen else part
            seen.add(h)
            value_v[b, n * tile_cols : (n + 1) * tile_cols, :] = jnp.where(
                head_lanes(b, h), values[:, block], 0.0
            ).astype(BF16)

    loads[5].wait()
    live = chain_s[0]
    for n in range(1, slots - 1):
        live = live + chain_s[n]
    key_live = iota((1, tile_cols), 1) + col * tile_cols < live
    lane = iota((1, LANES), 1)
    top = jnp.zeros((tile_rows, LANES), F32)
    for h in range(heads):
        scores = score_v[h] * scale + bias_v[pl.ds(h, tile_rows, stride=heads), :]
        scores = jnp.where(key_live, scores, MASKED)
        largest = jnp.maximum(jnp.max(scores, axis=-1, keepdims=True), FLOOR)
        weight_v[:, h * tile_cols : (h + 1) * tile_cols] = jnp.exp(scores - largest).astype(BF16)
        top = jnp.where(lax.rem(lane, heads) == h, largest, top)

    ones_row = lax.div(iota((heads * tile_cols, LANES), 0), tile_cols)
    ones_lane = iota((heads * tile_cols, LANES), 1)
    ones = jnp.where(
        (lax.rem(ones_lane, heads) == ones_row) & (ones_lane < 2 * heads), 1.0, 0.0
    ).astype(BF16)
    stats = jnp.where(lane < 2 * heads, matmul(weight_v[...], ones), top)
    first = stats.astype(BF16).astype(F32)
    second = (stats - first).astype(BF16).astype(F32)
    third = stats - first - second
    group = lax.div(lane, heads)
    stats = jnp.where(
        (group == 0) | (group == 2), first, jnp.where((group == 1) | (group == 3), second, third)
    )
    stats = jnp.where(group < 5, stats, 0.0).astype(BF16)
    own_rows = tile_rows // cols_n
    part_out[:, :, features:] = stats.astype(F32).reshape(cols_n, own_rows, LANES).astype(BF16)
    for b in range(lane_blocks):
        members = heads_of(b)
        summed = matmul(
            weight_v[:, members[0] * tile_cols : (members[-1] + 1) * tile_cols],
            value_v[b, : len(members) * tile_cols, :],
        )
        part_out[:, :, b * LANES : (b + 1) * LANES] = summed.reshape(
            cols_n, own_rows, LANES
        ).astype(BF16)

    part_in[pl.ds(col, 1)] = part_out[pl.ds(col, 1)]
    for d in far_first:
        part_copy(along(d)).start()
    loads[4].wait()
    spread_row = iota((LANES, features), 0)
    spread_head = lax.div(iota((LANES, features), 1), head_dim)
    matches = lax.rem(spread_row, heads) == spread_head
    spread_group = lax.div(spread_row, heads)
    to_total = jnp.where(matches & (spread_group < 2), 1.0, 0.0).astype(BF16)
    to_top = jnp.where(matches & (spread_group >= 2) & (spread_group < 5), 1.0, 0.0).astype(BF16)
    for d in far_first:
        landed(part_in, part_recv, along(d))
    arrived = flat(part_in[:, :, features:])
    total = matmul(arrived, to_total).reshape(cols_n, own_rows, features)
    tops = matmul(arrived, to_top).reshape(cols_n, own_rows, features)
    factor = jnp.exp(tops - jnp.max(tops, axis=0, keepdims=True))
    total = jnp.sum(factor * total, axis=0)
    numerator = jnp.sum(factor * part_in[:, :, :features].astype(F32), axis=0)
    attended = (own_gate * (numerator / total)).astype(BF16)
    out[...] = matmul(attended, out_proj_v[...]).astype(BF16)

    query_stage(wait_send)
    query_relay(1, wait_send)
    query_relay(-1, wait_send)
    key_stage(wait_send)
    key_relay(wait_send, False)

    for d in far_first:
        part_copy(along(d)).wait_send()


def shards(rows_n, cols_n, singles, pair, chain_sizes, single_proj, query_bias, pair_proj, out_proj):
    own, features = singles.shape
    tile_rows, tile_cols, channels = pair.shape
    heads = pair_proj.shape[1]
    chunks = 8
    reach = cols_n // 4
    dma = pltpu.SemaphoreType.DMA
    lane_blocks = features // LANES
    widest = -(-LANES // (features // heads)) + 1
    return pl.pallas_call(
        functools.partial(kernel, rows_n, cols_n, chunks),
        out_shape=pltpu.VMEM((own, features), BF16),
        in_specs=[pl.BlockSpec(memory_space=pl.ANY)] * 7,
        out_specs=pl.BlockSpec(memory_space=pltpu.VMEM),
        scratch_shapes=[
            pltpu.VMEM((own, features), BF16),
            pltpu.VMEM(pair.shape, BF16),
            pltpu.SMEM(chain_sizes.shape, jnp.int32),
            pltpu.VMEM(single_proj.shape, BF16),
            pltpu.VMEM((1, features), F32),
            pltpu.VMEM((heads, channels), BF16),
            pltpu.VMEM(out_proj.shape, BF16),
            pltpu.VMEM((cols_n, own, features), BF16),
            pltpu.VMEM((cols_n, own, features), BF16),
            pltpu.VMEM((tile_rows * heads, tile_cols), F32),
            pltpu.VMEM((heads, tile_rows, tile_cols), F32),
            pltpu.VMEM((tile_rows, heads * tile_cols), BF16),
            pltpu.VMEM((lane_blocks, widest * tile_cols, LANES), BF16),
            pltpu.VMEM((cols_n, own, features + LANES), BF16),
            pltpu.VMEM((cols_n, own, features + LANES), BF16),
            dma((6,)),
            dma((chunks,)),
            dma((2, cols_n)),
            dma((cols_n,)),
            dma((rows_n,)),
            dma((cols_n,)),
            pltpu.VMEM((cols_n, own, features), BF16),
            dma((cols_n,)),
            dma((cols_n,)),
            dma((cols_n,)),
            dma((cols_n,)),
        ],
        compiler_params=pltpu.CompilerParams(collective_id=0, has_side_effects=True),
    )(singles, pair, chain_sizes, single_proj, query_bias, pair_proj.T, out_proj)


def solution(mesh):
    placed = (
        P(("parts", "rows", "cols"), None),
        P(("parts", "rows"), "cols", None),
        P("parts"),
        P(),
        P(),
        P(),
        P(),
    )
    return jax.shard_map(
        functools.partial(shards, mesh.shape["rows"], mesh.shape["cols"]),
        mesh=mesh,
        in_specs=placed,
        out_specs=P(("parts", "rows", "cols"), None),
        check_vma=False,
    )
```

```python
import functools

import jax
import jax.numpy as jnp
from jax import lax
from jax.experimental import pallas as pl
from jax.experimental.pallas import tpu as pltpu
from jax.sharding import PartitionSpec as P

LANES = 128
MASKED = -1e30
FLOOR = -1e28
F32 = jnp.float32
BF16 = jnp.bfloat16


def peer(axis, index):
    return dict(device_id={axis: index}, device_id_type=pl.DeviceIdType.MESH)


def normalize(rows, axis):
    centered = rows - jnp.mean(rows, axis=axis, keepdims=True)
    variance = jnp.mean(centered * centered, axis=axis, keepdims=True)
    return centered * lax.rsqrt(variance + 1e-05)


def matmul(a, b):
    return jnp.dot(a, b, preferred_element_type=F32)


def iota(shape, dim):
    return lax.broadcasted_iota(jnp.int32, shape, dim)


def flat(blocks):
    count, rows, width = blocks.shape
    return blocks.astype(F32).reshape(count * rows, width).astype(BF16)


def kernel(
    rows_n,
    cols_n,
    chunks,
    singles,
    pair,
    chain,
    proj,
    q_bias,
    pair_proj,
    out_proj,
    out,
    own_v,
    pair_v,
    chain_s,
    proj_v,
    q_bias_v,
    pair_proj_v,
    out_proj_v,
    query_in,
    row_in,
    key_in,
    bias_v,
    score_v,
    stack_v,
    ones_v,
    weight_v,
    value_v,
    part_out,
    part_in,
    load_sem,
    pair_sem,
    query_send,
    query_recv,
    row_send,
    row_recv,
    key_send,
    key_recv,
    up_in,
    up_send,
    up_recv,
    down_in,
    down_send,
    down_recv,
    twin_send,
    twin_recv,
    part_send,
    part_recv,
):
    own, features = own_v.shape
    tile_rows, tile_cols, channels = pair_v.shape
    heads = pair_proj_v.shape[0]
    head_dim = features // heads
    lane_blocks = features // LANES
    slots = chain_s.shape[0]
    scale = head_dim ** (-0.5)
    row = lax.axis_index("rows")
    col = lax.axis_index("cols")

    loads = [
        pltpu.make_async_copy(src, dst, load_sem.at[n])
        for n, (src, dst) in enumerate(
            [
                (singles, own_v),
                (pair_proj, pair_proj_v),
                (proj, proj_v),
                (q_bias, q_bias_v.at[0]),
                (out_proj, out_proj_v),
                (chain, chain_s),
            ]
        )
    ]
    step = tile_rows // chunks
    pieces = [
        pltpu.make_async_copy(
            pair.at[pl.ds(n * step, step)], pair_v.at[pl.ds(n * step, step)], pair_sem.at[n]
        )
        for n in range(chunks)
    ]
    loads[0].start()
    loads[1].start()
    pieces[0].start()
    for load in loads[2:]:
        load.start()
    for piece in pieces[1:]:
        piece.start()

    reach = cols_n // 4
    core = lax.rem(row, 2)
    chips = rows_n // 2
    near = [d for n in range(reach, 0, -1) for d in (n, -n)]

    def along(d):
        return lax.rem(col + d + cols_n, cols_n)

    def across(d):
        return lax.rem(row + 2 * d, rows_n)

    def mine(target):
        return lax.rem(target, 2) == core

    barrier = pltpu.get_barrier_semaphore()
    for d in near:
        pl.semaphore_signal(barrier, inc=1, **peer("cols", along(d)))
    for d in range(1, chips):
        pl.semaphore_signal(barrier, inc=1, **peer("rows", across(d)))
    twin = row + 1 - 2 * core
    pl.semaphore_signal(barrier, inc=1, **peer("rows", twin))

    def send(src, dst, sent, arrived, axis, index):
        return pltpu.make_async_remote_copy(
            src_ref=src, dst_ref=dst, send_sem=sent, recv_sem=arrived, **peer(axis, index)
        )

    def query_copy(slot, target, stage):
        return send(
            query_in.at[slot],
            query_in.at[slot],
            query_send.at[stage, target],
            query_recv.at[slot],
            "cols",
            target,
        )

    def row_copy(target):
        return send(
            row_in.at[row], row_in.at[row], row_send.at[target], row_recv.at[row], "rows", target
        )

    def key_copy(src, slot, target, stage):
        return send(
            src, key_in.at[slot], key_send.at[stage, target], key_recv.at[slot], "cols", target
        )

    def up_copy(n):
        return send(
            row_in.at[along(reach + 1 + n)],
            up_in.at[n],
            up_send.at[n],
            up_recv.at[n],
            "cols",
            along(reach),
        )

    def down_copy(n):
        return send(
            row_in.at[along(-reach - 1 - n)],
            down_in.at[n],
            down_send.at[n],
            down_recv.at[n],
            "cols",
            along(-reach),
        )

    def twin_copy():
        return send(key_in, key_in, twin_send, twin_recv, "rows", twin)

    def part_copy(piece, other):
        tiles = pl.ds(piece, 1 if piece < lane_blocks - 1 else 2)
        return send(
            part_out.at[other, tiles],
            part_in.at[col, tiles],
            part_send.at[piece, other],
            part_recv.at[piece, col],
            "cols",
            other,
        )

    def part_arrival(piece, other):
        tiles = pl.ds(piece, 1 if piece < lane_blocks - 1 else 2)
        return send(
            part_in.at[other, tiles],
            part_in.at[other, tiles],
            part_send.at[piece, other],
            part_recv.at[piece, other],
            "cols",
            other,
        )

    def row_arrival(target):
        return send(
            row_in.at[target],
            row_in.at[target],
            row_send.at[target],
            row_recv.at[target],
            "rows",
            target,
        )

    def query_stage(act):
        for d in near:
            act(query_copy(col, along(d), 0))

    def query_relay(direction, act):
        for n in range(reach if direction > 0 else reach - 1, 0, -1):
            act(query_copy(along(-direction * reach), along(direction * n), 1))

    def key_stage(act, wait):
        def pass_on(target, copy):
            @pl.when(mine(target))
            def _():
                if wait:

                    @pl.when(target != row)
                    def _():
                        row_arrival(target).wait_recv()

                act(copy)

        for n in range(reach - 1, -1, -1):
            pass_on(along(reach + 1 + n), up_copy(n))
            if n < reach - 1:
                pass_on(along(-reach - 1 - n), down_copy(n))
        for d in near:
            target = along(d)
            pass_on(target, key_copy(row_in.at[target], col, target, 0))

    def key_relay(act, wait):
        for n in range(reach - 1, -1, -1):
            target = along(n + 1)

            @pl.when(mine(target))
            def _():
                if wait:
                    up_copy(n).wait_recv()
                act(key_copy(up_in.at[n], along(-reach), target, 1))

        for n in range(reach - 2, -1, -1):
            target = along(-n - 1)

            @pl.when(mine(target))
            def _():
                if wait:
                    down_copy(n).wait_recv()
                act(key_copy(down_in.at[n], along(reach), target, 1))

    def start(copy):
        copy.start()

    def wait_send(copy):
        copy.wait_send()

    far_first = sorted(range(1, cols_n), key=lambda d: -min(d, cols_n - d))

    loads[0].wait()
    normed = normalize(own_v[...].astype(F32), -1).astype(BF16)
    query_in[pl.ds(col, 1)] = normed[None]
    row_in[pl.ds(row, 1)] = normed[None]

    loads[1].wait()
    pair_w = pair_proj_v[...]

    def tile_bias(first, last):
        @pl.loop(first, last, unroll=4)
        def _(i):
            block = jnp.transpose(pair_v[i]).astype(F32)
            block_normed = normalize(block, 0).astype(BF16)
            bias = matmul(pair_w, block_normed)
            bias_v[pl.ds(pl.multiple_of(i * heads, heads), heads), :] = bias.astype(BF16).astype(F32)

    def bias_chunks(first, last):
        for n in range(first, last):
            pieces[n].wait()
            tile_bias(n * step, (n + 1) * step)

    pl.semaphore_wait(barrier, len(near) + chips)
    for d in range(1, chips):
        row_copy(across(d)).start()
    query_stage(start)
    bias_chunks(0, chunks // 2)

    query_copy(along(-reach), along(-reach), 0).wait_recv()
    query_relay(1, start)
    query_copy(along(reach), along(reach), 0).wait_recv()
    query_relay(-1, start)
    key_stage(start, True)

    @pl.when(mine(col))
    def _():
        @pl.when(col != row)
        def _():
            row_arrival(col).wait_recv()

        key_in[pl.ds(col, 1)] = row_in[pl.ds(col, 1)]

    loads[2].wait()
    loads[3].wait()
    own_gate = jax.nn.sigmoid(matmul(normed, proj_v[:, 3 * features :]))
    bias_chunks(chunks // 2, 3 * chunks // 4)
    key_relay(start, True)
    bias_chunks(3 * chunks // 4, chunks)

    def blocks_of(h):
        return range(h * head_dim // LANES, ((h + 1) * head_dim - 1) // LANES + 1)

    def head_lanes(b, h):
        feature = iota((1, LANES), 1) + b * LANES
        return (feature >= h * head_dim) & (feature < (h + 1) * head_dim)

    def lanes_of(b):
        return slice(b * LANES, (b + 1) * LANES)

    members = [[h for h in range(heads) if b in blocks_of(h)] for b in range(lane_blocks)]
    fresh = [[h for h in members[b] if blocks_of(h)[0] == b] for b in range(lane_blocks)]
    crossing = [[h for h in fresh[b] if blocks_of(h)[-1] > b] for b in range(lane_blocks)]

    loads[5].wait()
    live = chain_s[0]
    for n in range(1, slots - 1):
        live = live + chain_s[n]
    key_live = iota((1, tile_cols), 1) + col * tile_cols < live
    lane = iota((1, LANES), 1)
    ones_head = lax.div(iota((heads * tile_cols, LANES), 0), tile_cols)
    ones_lane = iota((heads * tile_cols, LANES), 1)
    ones_v[...] = jnp.where(
        (lax.rem(ones_lane, heads) == ones_head) & (ones_lane < 2 * heads), 1.0, 0.0
    ).astype(BF16)
    for h in range(heads):
        score_v[h] = jnp.where(key_live, bias_v[pl.ds(h, tile_rows, stride=heads), :], MASKED)

    for d in far_first:
        if d not in (reach, cols_n - reach):
            query_copy(along(d), along(d), 0).wait_recv()
    queries = (
        matmul(flat(query_in[...]), proj_v[:, :features]) + q_bias_v[...]
    ).astype(BF16).astype(F32)
    for b in range(lane_blocks):
        for n, h in enumerate(fresh[b]):
            stack_v[b, n * tile_rows : (n + 1) * tile_rows, :] = jnp.where(
                head_lanes(b, h), queries[:, lanes_of(b)], 0.0
            ).astype(BF16)
        for n, h in enumerate(crossing[b], len(fresh[b])):
            stack_v[b, n * tile_rows : (n + 1) * tile_rows, :] = jnp.where(
                head_lanes(b + 1, h), queries[:, lanes_of(b + 1)], 0.0
            ).astype(BF16)

    @pl.when(mine(col))
    def _():
        for d in far_first:
            key_copy(key_in.at[along(d)], along(d), along(d), 0).wait_recv()
        twin_copy().start()

    @pl.when(jnp.logical_not(mine(col)))
    def _():
        twin_copy().wait_recv()

    key_side = matmul(flat(key_in[...]), proj_v[:, features : 3 * features]).astype(BF16)
    keys = key_side[:, :features]
    values = key_side[:, features:].astype(F32)

    def against_keys(stacked, b):
        return lax.dot_general(
            stacked, keys[:, lanes_of(b)], (((1,), (1,)), ((), ())), preferred_element_type=F32
        )

    own_rows = tile_rows // cols_n
    top = jnp.zeros((tile_rows, LANES), F32)
    summed_weights = jnp.zeros((tile_rows, LANES), F32)
    for b in range(lane_blocks):
        count = len(fresh[b])
        raw = against_keys(stack_v[b, : count * tile_rows, :], b)
        if crossing[b]:
            extra = against_keys(
                stack_v[b, count * tile_rows : (count + len(crossing[b])) * tile_rows, :], b + 1
            )
        for n, h in enumerate(fresh[b]):
            scores = raw[n * tile_rows : (n + 1) * tile_rows]
            if h in crossing[b]:
                at = crossing[b].index(h) * tile_rows
                scores = scores + extra[at : at + tile_rows]
            scores = scores * scale + score_v[h]
            largest = jnp.maximum(jnp.max(scores, axis=-1, keepdims=True), FLOOR)
            weight_v[:, h * tile_cols : (h + 1) * tile_cols] = jnp.exp(scores - largest).astype(BF16)
            top = jnp.where(lax.rem(lane, heads) == h, largest, top)
        for n, h in enumerate(members[b]):
            value_v[b, n * tile_cols : (n + 1) * tile_cols, :] = jnp.where(
                head_lanes(b, h), values[:, lanes_of(b)], 0.0
            ).astype(BF16)
        summed = matmul(
            weight_v[:, members[b][0] * tile_cols : (members[b][-1] + 1) * tile_cols],
            value_v[b, : len(members[b]) * tile_cols, :],
        )
        part_out[:, b] = summed.reshape(cols_n, own_rows, LANES).astype(BF16)
        span = slice(fresh[b][0] * tile_cols, (fresh[b][-1] + 1) * tile_cols)
        summed_weights = summed_weights + matmul(weight_v[:, span], ones_v[span, :])
        if b < lane_blocks - 1:
            for d in far_first:
                part_copy(b, along(d)).start()

    stats = jnp.where(lane < 2 * heads, summed_weights, top)
    first = stats.astype(BF16).astype(F32)
    second = (stats - first).astype(BF16).astype(F32)
    third = stats - first - second
    group = lax.div(lane, heads)
    stats = jnp.where(
        (group == 0) | (group == 2), first, jnp.where((group == 1) | (group == 3), second, third)
    )
    stats = jnp.where(group < 5, stats, 0.0)
    part_out[:, lane_blocks] = stats.reshape(cols_n, own_rows, LANES).astype(BF16)
    for d in far_first:
        part_copy(lane_blocks - 1, along(d)).start()
    part_in[pl.ds(col, 1)] = part_out[pl.ds(col, 1)]
    loads[4].wait()
    spread_row = iota((LANES, features), 0)
    spread_head = lax.div(iota((LANES, features), 1), head_dim)
    matches = lax.rem(spread_row, heads) == spread_head
    spread_group = lax.div(spread_row, heads)
    to_total = jnp.where(matches & (spread_group < 2), 1.0, 0.0).astype(BF16)
    to_top = jnp.where(matches & (spread_group >= 2) & (spread_group < 5), 1.0, 0.0).astype(BF16)
    for d in far_first:
        for piece in range(lane_blocks):
            part_arrival(piece, along(d)).wait_recv()
    arrived = flat(part_in[:, lane_blocks])
    total = matmul(arrived, to_total).reshape(cols_n, own_rows, features)
    tops = matmul(arrived, to_top).reshape(cols_n, own_rows, features)
    factor = jnp.exp(tops - jnp.max(tops, axis=0, keepdims=True))
    total = jnp.sum(factor * total, axis=0)
    numerator = jnp.concatenate(
        [
            jnp.sum(factor[:, :, lanes_of(b)] * part_in[:, b].astype(F32), axis=0)
            for b in range(lane_blocks)
        ],
        axis=-1,
    )
    attended = (own_gate * (numerator / total)).astype(BF16)
    out[...] = matmul(attended, out_proj_v[...]).astype(BF16)

    for d in range(1, chips):
        row_copy(across(d)).wait_send()
    query_stage(wait_send)
    query_relay(1, wait_send)
    query_relay(-1, wait_send)
    key_stage(wait_send, False)
    key_relay(wait_send, False)

    @pl.when(mine(col))
    def _():
        twin_copy().wait_send()

    for d in far_first:
        for piece in range(lane_blocks):
            part_copy(piece, along(d)).wait_send()


def shards(rows_n, cols_n, singles, pair, chain_sizes, single_proj, query_bias, pair_proj, out_proj):
    own, features = singles.shape
    tile_rows, tile_cols, channels = pair.shape
    heads = pair_proj.shape[1]
    chunks = 8
    reach = cols_n // 4
    dma = pltpu.SemaphoreType.DMA
    lane_blocks = features // LANES
    widest = -(-LANES // (features // heads)) + 1
    return pl.pallas_call(
        functools.partial(kernel, rows_n, cols_n, chunks),
        out_shape=pltpu.VMEM((own, features), BF16),
        in_specs=[pl.BlockSpec(memory_space=pl.ANY)] * 7,
        out_specs=pl.BlockSpec(memory_space=pltpu.VMEM),
        scratch_shapes=[
            pltpu.VMEM((own, features), BF16),
            pltpu.VMEM(pair.shape, BF16),
            pltpu.SMEM(chain_sizes.shape, jnp.int32),
            pltpu.VMEM(single_proj.shape, BF16),
            pltpu.VMEM((1, features), F32),
            pltpu.VMEM((heads, channels), BF16),
            pltpu.VMEM(out_proj.shape, BF16),
            pltpu.VMEM((cols_n, own, features), BF16),
            pltpu.VMEM((rows_n, own, features), BF16),
            pltpu.VMEM((cols_n, own, features), BF16),
            pltpu.VMEM((tile_rows * heads, tile_cols), F32),
            pltpu.VMEM((heads, tile_rows, tile_cols), F32),
            pltpu.VMEM((lane_blocks, widest * tile_rows, LANES), BF16),
            pltpu.VMEM((heads * tile_cols, LANES), BF16),
            pltpu.VMEM((tile_rows, heads * tile_cols), BF16),
            pltpu.VMEM((lane_blocks, widest * tile_cols, LANES), BF16),
            pltpu.VMEM((cols_n, lane_blocks + 1, own, LANES), BF16),
            pltpu.VMEM((cols_n, lane_blocks + 1, own, LANES), BF16),
            dma((6,)),
            dma((chunks,)),
            dma((2, cols_n)),
            dma((cols_n,)),
            dma((rows_n,)),
            dma((rows_n,)),
            dma((2, cols_n)),
            dma((cols_n,)),
            pltpu.VMEM((reach, own, features), BF16),
            dma((reach,)),
            dma((reach,)),
            pltpu.VMEM((reach, own, features), BF16),
            dma((reach,)),
            dma((reach,)),
            dma,
            dma,
            dma((lane_blocks, cols_n)),
            dma((lane_blocks, cols_n)),
        ],
        compiler_params=pltpu.CompilerParams(collective_id=0, has_side_effects=True),
    )(singles, pair, chain_sizes, single_proj, query_bias, pair_proj.T, out_proj)


def solution(mesh):
    placed = (
        P(("parts", "rows", "cols"), None),
        P(("parts", "rows"), "cols", None),
        P("parts"),
        P(),
        P(),
        P(),
        P(),
    )
    return jax.shard_map(
        functools.partial(shards, mesh.shape["rows"], mesh.shape["cols"]),
        mesh=mesh,
        in_specs=placed,
        out_specs=P(("parts", "rows", "cols"), None),
        check_vma=False,
    )
```

```python
import functools

import jax
import jax.numpy as jnp
from jax import lax
from jax.experimental import pallas as pl
from jax.experimental.pallas import tpu as pltpu
from jax.sharding import PartitionSpec as P

LANES = 128
MASKED = -1e30
FLOOR = -1e28
F32 = jnp.float32
BF16 = jnp.bfloat16


def peer(axis, index):
    return dict(device_id={axis: index}, device_id_type=pl.DeviceIdType.MESH)


def normalize(rows, axis):
    centered = rows - jnp.mean(rows, axis=axis, keepdims=True)
    variance = jnp.mean(centered * centered, axis=axis, keepdims=True)
    return centered * lax.rsqrt(variance + 1e-05)


def matmul(a, b):
    return jnp.dot(a, b, preferred_element_type=F32)


def iota(shape, dim):
    return lax.broadcasted_iota(jnp.int32, shape, dim)


def flat(blocks):
    count, rows, width = blocks.shape
    return blocks.astype(F32).reshape(count * rows, width).astype(BF16)


def kernel(
    rows_n,
    cols_n,
    chunks,
    singles,
    pair,
    chain,
    proj,
    q_bias,
    pair_proj,
    out_proj,
    out,
    own_v,
    pair_v,
    chain_s,
    proj_v,
    q_bias_v,
    pair_proj_v,
    out_proj_v,
    query_in,
    row_in,
    key_in,
    bias_v,
    score_v,
    stack_v,
    ones_v,
    weight_v,
    value_v,
    part_out,
    part_in,
    load_sem,
    pair_sem,
    query_send,
    query_recv,
    row_send,
    row_recv,
    key_send,
    key_recv,
    up_in,
    up_send,
    up_recv,
    down_in,
    down_send,
    down_recv,
    twin_send,
    part_send,
    part_recv,
):
    own, features = own_v.shape
    tile_rows, tile_cols, channels = pair_v.shape
    heads = pair_proj_v.shape[0]
    head_dim = features // heads
    lane_blocks = features // LANES
    slots = chain_s.shape[0]
    scale = head_dim ** (-0.5)
    row = lax.axis_index("rows")
    col = lax.axis_index("cols")

    loads = [
        pltpu.make_async_copy(src, dst, load_sem.at[n])
        for n, (src, dst) in enumerate(
            [
                (singles, own_v),
                (pair_proj, pair_proj_v),
                (proj, proj_v),
                (q_bias, q_bias_v.at[0]),
                (out_proj, out_proj_v),
                (chain, chain_s),
            ]
        )
    ]
    step = tile_rows // chunks

    def piece(n):
        rows = pl.ds(pl.multiple_of(n * step, step), step)
        return pltpu.make_async_copy(pair.at[rows], pair_v.at[rows], pair_sem.at[n])

    loads[0].start()
    loads[1].start()
    piece(0).start()
    for load in loads[2:]:
        load.start()
    for n in range(1, chunks):
        piece(n).start()

    reach = cols_n // 4
    core = lax.rem(row, 2)
    chips = rows_n // 2
    near = [d for n in range(reach, 0, -1) for d in (n, -n)]

    def along(d):
        return lax.rem(col + d + cols_n, cols_n)

    def across(d):
        return lax.rem(row + 2 * d, rows_n)

    def mine(target):
        return lax.rem(target, 2) == core

    barrier = pltpu.get_barrier_semaphore()
    for d in near:
        pl.semaphore_signal(barrier, inc=1, **peer("cols", along(d)))
    for d in range(1, chips):
        pl.semaphore_signal(barrier, inc=1, **peer("rows", across(d)))
    twin = row + 1 - 2 * core
    pl.semaphore_signal(barrier, inc=1, **peer("rows", twin))

    def send(src, dst, sent, arrived, axis, index):
        return pltpu.make_async_remote_copy(
            src_ref=src, dst_ref=dst, send_sem=sent, recv_sem=arrived, **peer(axis, index)
        )

    def query_copy(slot, target, stage):
        return send(
            query_in.at[slot],
            query_in.at[slot],
            query_send.at[stage, target],
            query_recv.at[slot],
            "cols",
            target,
        )

    def row_copy(target):
        return send(
            row_in.at[row], row_in.at[row], row_send.at[target], row_recv.at[row], "rows", target
        )

    def key_copy(src, slot, target, stage):
        return send(
            src, key_in.at[slot], key_send.at[stage, target], key_recv.at[slot], "cols", target
        )

    def up_copy(n):
        return send(
            row_in.at[along(reach + 1 + n)],
            up_in.at[n],
            up_send.at[n],
            up_recv.at[n],
            "cols",
            along(reach),
        )

    def down_copy(n):
        return send(
            row_in.at[along(-reach - 1 - n)],
            down_in.at[n],
            down_send.at[n],
            down_recv.at[n],
            "cols",
            along(-reach),
        )

    def twin_copy(slot):
        return send(
            key_in.at[slot], key_in.at[slot], twin_send.at[slot], key_recv.at[slot], "rows", twin
        )

    def part_copy(piece, other):
        tiles = pl.ds(piece, 1 if piece < lane_blocks - 1 else 2)
        return send(
            part_out.at[other, tiles],
            part_in.at[col, tiles],
            part_send.at[piece, other],
            part_recv.at[piece, col],
            "cols",
            other,
        )

    def part_arrival(piece, other):
        tiles = pl.ds(piece, 1 if piece < lane_blocks - 1 else 2)
        return send(
            part_in.at[other, tiles],
            part_in.at[other, tiles],
            part_send.at[piece, other],
            part_recv.at[piece, other],
            "cols",
            other,
        )

    def row_arrival(target):
        return send(
            row_in.at[target],
            row_in.at[target],
            row_send.at[target],
            row_recv.at[target],
            "rows",
            target,
        )

    def query_stage(act):
        for d in near:
            act(query_copy(col, along(d), 0))

    def query_relay(direction, act):
        for n in range(reach if direction > 0 else reach - 1, 0, -1):
            act(query_copy(along(-direction * reach), along(direction * n), 1))

    def key_stage(act, wait):
        def pass_on(target, copy):
            @pl.when(mine(target))
            def _():
                if wait:

                    @pl.when(target != row)
                    def _():
                        row_arrival(target).wait_recv()

                act(copy)

        for n in range(reach - 1, -1, -1):
            pass_on(along(reach + 1 + n), up_copy(n))
            if n < reach - 1:
                pass_on(along(-reach - 1 - n), down_copy(n))
        for d in near:
            target = along(d)
            pass_on(target, key_copy(row_in.at[target], col, target, 0))

    def key_relay(act, wait):
        for n in range(reach - 1, -1, -1):
            target = along(n + 1)

            @pl.when(mine(target))
            def _():
                if wait:
                    up_copy(n).wait_recv()
                act(key_copy(up_in.at[n], along(-reach), target, 1))

        for n in range(reach - 2, -1, -1):
            target = along(-n - 1)

            @pl.when(mine(target))
            def _():
                if wait:
                    down_copy(n).wait_recv()
                act(key_copy(down_in.at[n], along(reach), target, 1))

    def start(copy):
        copy.start()

    def wait_send(copy):
        copy.wait_send()

    far_first = sorted(range(1, cols_n), key=lambda d: -min(d, cols_n - d))

    loads[0].wait()
    normed = normalize(own_v[...].astype(F32), -1).astype(BF16)
    query_in[pl.ds(col, 1)] = normed[None]
    row_in[pl.ds(row, 1)] = normed[None]

    loads[1].wait()
    pair_w = pair_proj_v[...]

    def bias_chunks(first, last):
        @pl.loop(first, last)
        def _(n):
            piece(n).wait()
            for m in range(step):
                i = n * step + m
                block = jnp.transpose(pair_v[i]).astype(F32)
                bias = matmul(pair_w, normalize(block, 0).astype(BF16))
                bias_v[pl.ds(pl.multiple_of(i * heads, heads), heads), :] = bias.astype(BF16).astype(F32)

    bias_chunks(0, chunks // 4)
    pl.semaphore_wait(barrier, len(near) + chips)
    for d in range(1, chips):
        row_copy(across(d)).start()
    query_stage(start)
    bias_chunks(chunks // 4, 3 * chunks // 4)

    key_stage(start, True)
    query_copy(along(-reach), along(-reach), 0).wait_recv()
    query_relay(1, start)
    query_copy(along(reach), along(reach), 0).wait_recv()
    query_relay(-1, start)

    @pl.when(mine(col))
    def _():
        @pl.when(col != row)
        def _():
            row_arrival(col).wait_recv()

        key_in[pl.ds(col, 1)] = row_in[pl.ds(col, 1)]

    loads[2].wait()
    loads[3].wait()
    own_gate = jax.nn.sigmoid(matmul(normed, proj_v[:, 3 * features :]))
    bias_chunks(3 * chunks // 4, chunks)
    key_relay(start, True)

    def blocks_of(h):
        return range(h * head_dim // LANES, ((h + 1) * head_dim - 1) // LANES + 1)

    def head_lanes(b, h):
        feature = iota((1, LANES), 1) + b * LANES
        return (feature >= h * head_dim) & (feature < (h + 1) * head_dim)

    def lanes_of(b):
        return slice(b * LANES, (b + 1) * LANES)

    members = [[h for h in range(heads) if b in blocks_of(h)] for b in range(lane_blocks)]
    fresh = [[h for h in members[b] if blocks_of(h)[0] == b] for b in range(lane_blocks)]
    crossing = [[h for h in fresh[b] if blocks_of(h)[-1] > b] for b in range(lane_blocks)]

    loads[5].wait()
    live = chain_s[0]
    for n in range(1, slots - 1):
        live = live + chain_s[n]
    key_live = iota((1, tile_cols), 1) + col * tile_cols < live
    lane = iota((1, LANES), 1)
    ones_head = lax.div(iota((heads * tile_cols, LANES), 0), tile_cols)
    ones_lane = iota((heads * tile_cols, LANES), 1)
    ones_v[...] = jnp.where(
        (lax.rem(ones_lane, heads) == ones_head) & (ones_lane < 2 * heads), 1.0, 0.0
    ).astype(BF16)
    for h in range(heads):
        score_v[h] = jnp.where(key_live, bias_v[pl.ds(h, tile_rows, stride=heads), :], MASKED)

    for d in far_first:
        if d not in (reach, cols_n - reach):
            query_copy(along(d), along(d), 0).wait_recv()
    queries = (
        matmul(flat(query_in[...]), proj_v[:, :features]) + q_bias_v[...]
    ).astype(BF16).astype(F32)
    for b in range(lane_blocks):
        for n, h in enumerate(fresh[b]):
            stack_v[b, n * tile_rows : (n + 1) * tile_rows, :] = jnp.where(
                head_lanes(b, h), queries[:, lanes_of(b)], 0.0
            ).astype(BF16)
        for n, h in enumerate(crossing[b], len(fresh[b])):
            stack_v[b, n * tile_rows : (n + 1) * tile_rows, :] = jnp.where(
                head_lanes(b + 1, h), queries[:, lanes_of(b + 1)], 0.0
            ).astype(BF16)

    @pl.when(mine(col))
    def _():
        twin_copy(col).start()
        for d in far_first:
            key_copy(key_in.at[along(d)], along(d), along(d), 0).wait_recv()
            twin_copy(along(d)).start()

    @pl.when(jnp.logical_not(mine(col)))
    def _():
        for d in range(cols_n):
            twin_copy(along(d)).wait_recv()

    key_side = matmul(flat(key_in[...]), proj_v[:, features : 3 * features]).astype(BF16)
    keys = key_side[:, :features]
    values = key_side[:, features:].astype(F32)

    def against_keys(stacked, b):
        return lax.dot_general(
            stacked, keys[:, lanes_of(b)], (((1,), (1,)), ((), ())), preferred_element_type=F32
        )

    own_rows = tile_rows // cols_n
    top = jnp.zeros((tile_rows, LANES), F32)
    summed_weights = jnp.zeros((tile_rows, LANES), F32)
    for b in range(lane_blocks):
        count = len(fresh[b])
        raw = against_keys(stack_v[b, : count * tile_rows, :], b)
        if crossing[b]:
            extra = against_keys(
                stack_v[b, count * tile_rows : (count + len(crossing[b])) * tile_rows, :], b + 1
            )
        for n, h in enumerate(fresh[b]):
            scores = raw[n * tile_rows : (n + 1) * tile_rows]
            if h in crossing[b]:
                at = crossing[b].index(h) * tile_rows
                scores = scores + extra[at : at + tile_rows]
            scores = scores * scale + score_v[h]
            largest = jnp.maximum(jnp.max(scores, axis=-1, keepdims=True), FLOOR)
            weight_v[:, h * tile_cols : (h + 1) * tile_cols] = jnp.exp(scores - largest).astype(BF16)
            top = jnp.where(lax.rem(lane, heads) == h, largest, top)
        for n, h in enumerate(members[b]):
            value_v[b, n * tile_cols : (n + 1) * tile_cols, :] = jnp.where(
                head_lanes(b, h), values[:, lanes_of(b)], 0.0
            ).astype(BF16)
        summed = matmul(
            weight_v[:, members[b][0] * tile_cols : (members[b][-1] + 1) * tile_cols],
            value_v[b, : len(members[b]) * tile_cols, :],
        )
        part_out[:, b] = summed.reshape(cols_n, own_rows, LANES).astype(BF16)
        span = slice(fresh[b][0] * tile_cols, (fresh[b][-1] + 1) * tile_cols)
        summed_weights = summed_weights + matmul(weight_v[:, span], ones_v[span, :])
        if b < lane_blocks - 1:
            for d in far_first:
                part_copy(b, along(d)).start()

    stats = jnp.where(lane < 2 * heads, summed_weights, top)
    first = stats.astype(BF16).astype(F32)
    second = (stats - first).astype(BF16).astype(F32)
    third = stats - first - second
    group = lax.div(lane, heads)
    stats = jnp.where(
        (group == 0) | (group == 2), first, jnp.where((group == 1) | (group == 3), second, third)
    )
    stats = jnp.where(group < 5, stats, 0.0)
    part_out[:, lane_blocks] = stats.reshape(cols_n, own_rows, LANES).astype(BF16)
    for d in far_first:
        part_copy(lane_blocks - 1, along(d)).start()
    part_in[pl.ds(col, 1)] = part_out[pl.ds(col, 1)]
    loads[4].wait()
    spread_row = iota((LANES, features), 0)
    spread_head = lax.div(iota((LANES, features), 1), head_dim)
    matches = lax.rem(spread_row, heads) == spread_head
    spread_group = lax.div(spread_row, heads)
    to_total = jnp.where(matches & (spread_group < 2), 1.0, 0.0).astype(BF16)
    to_top = jnp.where(matches & (spread_group >= 2) & (spread_group < 5), 1.0, 0.0).astype(BF16)
    for d in far_first:
        for piece in range(lane_blocks):
            part_arrival(piece, along(d)).wait_recv()
    arrived = flat(part_in[:, lane_blocks])
    total = matmul(arrived, to_total).reshape(cols_n, own_rows, features)
    tops = matmul(arrived, to_top).reshape(cols_n, own_rows, features)
    factor = jnp.exp(tops - jnp.max(tops, axis=0, keepdims=True))
    total = jnp.sum(factor * total, axis=0)
    numerator = jnp.concatenate(
        [
            jnp.sum(factor[:, :, lanes_of(b)] * part_in[:, b].astype(F32), axis=0)
            for b in range(lane_blocks)
        ],
        axis=-1,
    )
    attended = (own_gate * (numerator / total)).astype(BF16)
    out[...] = matmul(attended, out_proj_v[...]).astype(BF16)

    for d in range(1, chips):
        row_copy(across(d)).wait_send()
    query_stage(wait_send)
    query_relay(1, wait_send)
    query_relay(-1, wait_send)
    key_stage(wait_send, False)
    key_relay(wait_send, False)

    @pl.when(mine(col))
    def _():
        for d in range(cols_n):
            twin_copy(along(d)).wait_send()

    for d in far_first:
        for piece in range(lane_blocks):
            part_copy(piece, along(d)).wait_send()


def shards(rows_n, cols_n, singles, pair, chain_sizes, single_proj, query_bias, pair_proj, out_proj):
    own, features = singles.shape
    tile_rows, tile_cols, channels = pair.shape
    heads = pair_proj.shape[1]
    chunks = 8
    reach = cols_n // 4
    dma = pltpu.SemaphoreType.DMA
    lane_blocks = features // LANES
    widest = -(-LANES // (features // heads)) + 1
    return pl.pallas_call(
        functools.partial(kernel, rows_n, cols_n, chunks),
        out_shape=pltpu.VMEM((own, features), BF16),
        in_specs=[pl.BlockSpec(memory_space=pl.ANY)] * 7,
        out_specs=pl.BlockSpec(memory_space=pltpu.VMEM),
        scratch_shapes=[
            pltpu.VMEM((own, features), BF16),
            pltpu.VMEM(pair.shape, BF16),
            pltpu.SMEM(chain_sizes.shape, jnp.int32),
            pltpu.VMEM(single_proj.shape, BF16),
            pltpu.VMEM((1, features), F32),
            pltpu.VMEM((heads, channels), BF16),
            pltpu.VMEM(out_proj.shape, BF16),
            pltpu.VMEM((cols_n, own, features), BF16),
            pltpu.VMEM((rows_n, own, features), BF16),
            pltpu.VMEM((cols_n, own, features), BF16),
            pltpu.VMEM((tile_rows * heads, tile_cols), F32),
            pltpu.VMEM((heads, tile_rows, tile_cols), F32),
            pltpu.VMEM((lane_blocks, widest * tile_rows, LANES), BF16),
            pltpu.VMEM((heads * tile_cols, LANES), BF16),
            pltpu.VMEM((tile_rows, heads * tile_cols), BF16),
            pltpu.VMEM((lane_blocks, widest * tile_cols, LANES), BF16),
            pltpu.VMEM((cols_n, lane_blocks + 1, own, LANES), BF16),
            pltpu.VMEM((cols_n, lane_blocks + 1, own, LANES), BF16),
            dma((6,)),
            dma((chunks,)),
            dma((2, cols_n)),
            dma((cols_n,)),
            dma((rows_n,)),
            dma((rows_n,)),
            dma((2, cols_n)),
            dma((cols_n,)),
            pltpu.VMEM((reach, own, features), BF16),
            dma((reach,)),
            dma((reach,)),
            pltpu.VMEM((reach, own, features), BF16),
            dma((reach,)),
            dma((reach,)),
            dma((cols_n,)),
            dma((lane_blocks, cols_n)),
            dma((lane_blocks, cols_n)),
        ],
        compiler_params=pltpu.CompilerParams(collective_id=0, has_side_effects=True),
    )(singles, pair, chain_sizes, single_proj, query_bias, pair_proj.T, out_proj)


def solution(mesh):
    placed = (
        P(("parts", "rows", "cols"), None),
        P(("parts", "rows"), "cols", None),
        P("parts"),
        P(),
        P(),
        P(),
        P(),
    )
    return jax.shard_map(
        functools.partial(shards, mesh.shape["rows"], mesh.shape["cols"]),
        mesh=mesh,
        in_specs=placed,
        out_specs=P(("parts", "rows", "cols"), None),
        check_vma=False,
    )
```

```python
import functools

import jax
import jax.numpy as jnp
from jax import lax
from jax.experimental import pallas as pl
from jax.experimental.pallas import tpu as pltpu
from jax.sharding import PartitionSpec as P

LANES = 128
MASKED = -1e30
FLOOR = -1e28
F32 = jnp.float32
BF16 = jnp.bfloat16


def peer(axis, index):
    return dict(device_id={axis: index}, device_id_type=pl.DeviceIdType.MESH)


def normalize(rows, axis):
    centered = rows - jnp.mean(rows, axis=axis, keepdims=True)
    variance = jnp.mean(centered * centered, axis=axis, keepdims=True)
    return centered * lax.rsqrt(variance + 1e-05)


def matmul(a, b):
    return jnp.dot(a, b, preferred_element_type=F32)


def iota(shape, dim):
    return lax.broadcasted_iota(jnp.int32, shape, dim)


def flat(blocks):
    count, rows, width = blocks.shape
    return blocks.astype(F32).reshape(count * rows, width).astype(BF16)


def kernel(
    rows_n,
    cols_n,
    chunks,
    singles,
    pair,
    chain,
    proj,
    q_bias,
    pair_proj,
    out_proj,
    out,
    own_v,
    pair_v,
    chain_s,
    proj_v,
    q_bias_v,
    pair_proj_v,
    out_proj_v,
    query_in,
    row_in,
    key_in,
    bias_v,
    score_v,
    stack_v,
    ones_v,
    weight_v,
    value_v,
    part_out,
    part_in,
    load_sem,
    pair_sem,
    query_send,
    query_recv,
    row_send,
    row_recv,
    key_send,
    key_recv,
    ready_up,
    ready_down,
    twin_send,
    part_send,
    part_recv,
):
    own, features = own_v.shape
    tile_rows, tile_cols, channels = pair_v.shape
    heads = pair_proj_v.shape[0]
    head_dim = features // heads
    lane_blocks = features // LANES
    slots = chain_s.shape[0]
    scale = head_dim ** (-0.5)
    row = lax.axis_index("rows")
    col = lax.axis_index("cols")

    loads = [
        pltpu.make_async_copy(src, dst, load_sem.at[n])
        for n, (src, dst) in enumerate(
            [
                (singles, own_v),
                (pair_proj, pair_proj_v),
                (proj, proj_v),
                (q_bias, q_bias_v.at[0]),
                (out_proj, out_proj_v),
                (chain, chain_s),
            ]
        )
    ]
    step = tile_rows // chunks

    def piece(n):
        rows = pl.ds(pl.multiple_of(n * step, step), step)
        return pltpu.make_async_copy(pair.at[rows], pair_v.at[rows], pair_sem.at[n])

    loads[0].start()
    loads[1].start()
    piece(0).start()
    for load in loads[2:]:
        load.start()
    for n in range(1, chunks):
        piece(n).start()

    reach = cols_n // 4
    core = lax.rem(row, 2)
    chips = rows_n // 2
    near = [d for n in range(reach, 0, -1) for d in (n, -n)]

    def along(d):
        return lax.rem(col + d + cols_n, cols_n)

    def across(d):
        return lax.rem(row + 2 * d, rows_n)

    def mine(target):
        return lax.rem(target, 2) == core

    barrier = pltpu.get_barrier_semaphore()
    for d in near:
        pl.semaphore_signal(barrier, inc=1, **peer("cols", along(d)))
    for d in range(1, chips):
        pl.semaphore_signal(barrier, inc=1, **peer("rows", across(d)))
    twin = row + 1 - 2 * core
    pl.semaphore_signal(barrier, inc=1, **peer("rows", twin))

    def send(src, dst, sent, arrived, axis, index):
        return pltpu.make_async_remote_copy(
            src_ref=src, dst_ref=dst, send_sem=sent, recv_sem=arrived, **peer(axis, index)
        )

    def query_copy(slot, target, stage):
        return send(
            query_in.at[slot],
            query_in.at[slot],
            query_send.at[stage, target],
            query_recv.at[slot],
            "cols",
            target,
        )

    def row_copy(target):
        return send(
            row_in.at[row], row_in.at[row], row_send.at[target], row_recv.at[row], "rows", target
        )

    def key_copy(src, slot, target):
        return send(
            row_in.at[src], key_in.at[slot], key_send.at[target], key_recv.at[slot], "cols", target
        )

    def twin_copy(slot):
        return send(
            key_in.at[slot], key_in.at[slot], twin_send.at[slot], key_recv.at[slot], "rows", twin
        )

    def part_copy(other):
        return send(
            part_out.at[other],
            part_in.at[col],
            part_send.at[other],
            part_recv.at[col],
            "cols",
            other,
        )

    def part_arrival(other):
        return send(
            part_in.at[other],
            part_in.at[other],
            part_send.at[other],
            part_recv.at[other],
            "cols",
            other,
        )

    def row_arrival(target):
        return send(
            row_in.at[target],
            row_in.at[target],
            row_send.at[target],
            row_recv.at[target],
            "rows",
            target,
        )

    def query_stage(act):
        for d in near:
            act(query_copy(col, along(d), 0))

    def query_relay(direction, act):
        for n in range(reach if direction > 0 else reach - 1, 0, -1):
            act(query_copy(along(-direction * reach), along(direction * n), 1))

    far_first = sorted(range(1, cols_n), key=lambda d: -min(d, cols_n - d))

    def key_stage(act, wait):
        def pass_on(target, copy):
            @pl.when(mine(target))
            def _():
                if wait:

                    @pl.when(target != row)
                    def _():
                        row_arrival(target).wait_recv()

                act(copy)

        if wait:
            pl.semaphore_wait(ready_up, 1)
            pl.semaphore_wait(ready_down, 1)
        for d in far_first:
            pass_on(along(d), key_copy(along(d), col, along(d)))

    def start(copy):
        copy.start()

    def wait_send(copy):
        copy.wait_send()


    loads[0].wait()
    normed = normalize(own_v[...].astype(F32), -1).astype(BF16)
    query_in[pl.ds(col, 1)] = normed[None]
    row_in[pl.ds(row, 1)] = normed[None]

    loads[1].wait()
    pair_w = pair_proj_v[...]

    def bias_chunks(first, last):
        @pl.loop(first, last)
        def _(n):
            piece(n).wait()
            for m in range(step):
                i = n * step + m
                block = jnp.transpose(pair_v[i]).astype(F32)
                bias = matmul(pair_w, normalize(block, 0).astype(BF16))
                bias_v[pl.ds(pl.multiple_of(i * heads, heads), heads), :] = bias.astype(BF16).astype(F32)

    bias_chunks(0, chunks // 4)
    pl.semaphore_wait(barrier, len(near) + chips)
    for d in range(1, chips):
        row_copy(across(d)).start()
    pl.semaphore_signal(ready_up, inc=1, **peer("cols", along(-reach)))
    pl.semaphore_signal(ready_down, inc=1, **peer("cols", along(reach)))
    query_stage(start)
    bias_chunks(chunks // 4, 5 * chunks // 8)

    key_stage(start, True)
    query_copy(along(-reach), along(-reach), 0).wait_recv()
    query_relay(1, start)
    query_copy(along(reach), along(reach), 0).wait_recv()
    query_relay(-1, start)

    @pl.when(mine(col))
    def _():
        @pl.when(col != row)
        def _():
            row_arrival(col).wait_recv()

        key_in[pl.ds(col, 1)] = row_in[pl.ds(col, 1)]

    loads[2].wait()
    loads[3].wait()
    own_gate = jax.nn.sigmoid(matmul(normed, proj_v[:, 3 * features :]))
    bias_chunks(5 * chunks // 8, chunks)

    def blocks_of(h):
        return range(h * head_dim // LANES, ((h + 1) * head_dim - 1) // LANES + 1)

    def head_lanes(b, h):
        feature = iota((1, LANES), 1) + b * LANES
        return (feature >= h * head_dim) & (feature < (h + 1) * head_dim)

    def lanes_of(b):
        return slice(b * LANES, (b + 1) * LANES)

    members = [[h for h in range(heads) if b in blocks_of(h)] for b in range(lane_blocks)]
    fresh = [[h for h in members[b] if blocks_of(h)[0] == b] for b in range(lane_blocks)]
    crossing = [[h for h in fresh[b] if blocks_of(h)[-1] > b] for b in range(lane_blocks)]

    loads[5].wait()
    live = chain_s[0]
    for n in range(1, slots - 1):
        live = live + chain_s[n]
    key_live = iota((1, tile_cols), 1) + col * tile_cols < live
    lane = iota((1, LANES), 1)
    ones_head = lax.div(iota((heads * tile_cols, LANES), 0), tile_cols)
    ones_lane = iota((heads * tile_cols, LANES), 1)
    ones_v[...] = jnp.where(
        (lax.rem(ones_lane, heads) == ones_head) & (ones_lane < 2 * heads), 1.0, 0.0
    ).astype(BF16)
    for h in range(heads):
        score_v[h] = jnp.where(key_live, bias_v[pl.ds(h, tile_rows, stride=heads), :], MASKED)

    for d in far_first:
        if d not in (reach, cols_n - reach):
            query_copy(along(d), along(d), 0).wait_recv()
    queries = (
        matmul(flat(query_in[...]), proj_v[:, :features]) + q_bias_v[...]
    ).astype(BF16).astype(F32)
    for b in range(lane_blocks):
        for n, h in enumerate(fresh[b]):
            stack_v[b, n * tile_rows : (n + 1) * tile_rows, :] = jnp.where(
                head_lanes(b, h), queries[:, lanes_of(b)], 0.0
            ).astype(BF16)
        for n, h in enumerate(crossing[b], len(fresh[b])):
            stack_v[b, n * tile_rows : (n + 1) * tile_rows, :] = jnp.where(
                head_lanes(b + 1, h), queries[:, lanes_of(b + 1)], 0.0
            ).astype(BF16)

    @pl.when(mine(col))
    def _():
        twin_copy(col).start()
        for d in far_first:
            key_copy(along(d), along(d), along(d)).wait_recv()
            twin_copy(along(d)).start()

    @pl.when(jnp.logical_not(mine(col)))
    def _():
        for d in range(cols_n):
            twin_copy(along(d)).wait_recv()

    key_side = matmul(flat(key_in[...]), proj_v[:, features : 3 * features]).astype(BF16)
    keys = key_side[:, :features]
    values = key_side[:, features:].astype(F32)

    def against_keys(stacked, b):
        return lax.dot_general(
            stacked, keys[:, lanes_of(b)], (((1,), (1,)), ((), ())), preferred_element_type=F32
        )

    own_rows = tile_rows // cols_n
    top = jnp.zeros((tile_rows, LANES), F32)
    summed_weights = jnp.zeros((tile_rows, LANES), F32)
    for b in range(lane_blocks):
        count = len(fresh[b])
        raw = against_keys(stack_v[b, : count * tile_rows, :], b)
        if crossing[b]:
            extra = against_keys(
                stack_v[b, count * tile_rows : (count + len(crossing[b])) * tile_rows, :], b + 1
            )
        for n, h in enumerate(fresh[b]):
            scores = raw[n * tile_rows : (n + 1) * tile_rows]
            if h in crossing[b]:
                at = crossing[b].index(h) * tile_rows
                scores = scores + extra[at : at + tile_rows]
            scores = scores * scale + score_v[h]
            largest = jnp.maximum(jnp.max(scores, axis=-1, keepdims=True), FLOOR)
            weight_v[:, h * tile_cols : (h + 1) * tile_cols] = jnp.exp(scores - largest).astype(BF16)
            top = jnp.where(lax.rem(lane, heads) == h, largest, top)
        for n, h in enumerate(members[b]):
            value_v[b, n * tile_cols : (n + 1) * tile_cols, :] = jnp.where(
                head_lanes(b, h), values[:, lanes_of(b)], 0.0
            ).astype(BF16)
        summed = matmul(
            weight_v[:, members[b][0] * tile_cols : (members[b][-1] + 1) * tile_cols],
            value_v[b, : len(members[b]) * tile_cols, :],
        )
        part_out[:, b] = summed.reshape(cols_n, own_rows, LANES).astype(BF16)
        span = slice(fresh[b][0] * tile_cols, (fresh[b][-1] + 1) * tile_cols)
        summed_weights = summed_weights + matmul(weight_v[:, span], ones_v[span, :])

    stats = jnp.where(lane < 2 * heads, summed_weights, top)
    first = stats.astype(BF16).astype(F32)
    second = (stats - first).astype(BF16).astype(F32)
    third = stats - first - second
    group = lax.div(lane, heads)
    stats = jnp.where(
        (group == 0) | (group == 2), first, jnp.where((group == 1) | (group == 3), second, third)
    )
    stats = jnp.where(group < 5, stats, 0.0)
    part_out[:, lane_blocks] = stats.reshape(cols_n, own_rows, LANES).astype(BF16)
    for d in far_first:
        part_copy(along(d)).start()
    part_in[pl.ds(col, 1)] = part_out[pl.ds(col, 1)]
    loads[4].wait()
    spread_row = iota((LANES, features), 0)
    spread_head = lax.div(iota((LANES, features), 1), head_dim)
    matches = lax.rem(spread_row, heads) == spread_head
    spread_group = lax.div(spread_row, heads)
    to_total = jnp.where(matches & (spread_group < 2), 1.0, 0.0).astype(BF16)
    to_top = jnp.where(matches & (spread_group >= 2) & (spread_group < 5), 1.0, 0.0).astype(BF16)
    for d in far_first:
        part_arrival(along(d)).wait_recv()
    arrived = flat(part_in[:, lane_blocks])
    total = matmul(arrived, to_total).reshape(cols_n, own_rows, features)
    tops = matmul(arrived, to_top).reshape(cols_n, own_rows, features)
    factor = jnp.exp(tops - jnp.max(tops, axis=0, keepdims=True))
    total = jnp.sum(factor * total, axis=0)
    numerator = jnp.concatenate(
        [
            jnp.sum(factor[:, :, lanes_of(b)] * part_in[:, b].astype(F32), axis=0)
            for b in range(lane_blocks)
        ],
        axis=-1,
    )
    attended = (own_gate * (numerator / total)).astype(BF16)
    out[...] = matmul(attended, out_proj_v[...]).astype(BF16)

    for d in range(1, chips):
        row_copy(across(d)).wait_send()
    query_stage(wait_send)
    query_relay(1, wait_send)
    query_relay(-1, wait_send)
    key_stage(wait_send, False)

    @pl.when(mine(col))
    def _():
        for d in range(cols_n):
            twin_copy(along(d)).wait_send()

    for d in far_first:
        part_copy(along(d)).wait_send()


def shards(rows_n, cols_n, singles, pair, chain_sizes, single_proj, query_bias, pair_proj, out_proj):
    own, features = singles.shape
    tile_rows, tile_cols, channels = pair.shape
    heads = pair_proj.shape[1]
    chunks = 8
    dma = pltpu.SemaphoreType.DMA
    lane_blocks = features // LANES
    widest = -(-LANES // (features // heads)) + 1
    return pl.pallas_call(
        functools.partial(kernel, rows_n, cols_n, chunks),
        out_shape=pltpu.VMEM((own, features), BF16),
        in_specs=[pl.BlockSpec(memory_space=pl.ANY)] * 7,
        out_specs=pl.BlockSpec(memory_space=pltpu.VMEM),
        scratch_shapes=[
            pltpu.VMEM((own, features), BF16),
            pltpu.VMEM(pair.shape, BF16),
            pltpu.SMEM(chain_sizes.shape, jnp.int32),
            pltpu.VMEM(single_proj.shape, BF16),
            pltpu.VMEM((1, features), F32),
            pltpu.VMEM((heads, channels), BF16),
            pltpu.VMEM(out_proj.shape, BF16),
            pltpu.VMEM((cols_n, own, features), BF16),
            pltpu.VMEM((rows_n, own, features), BF16),
            pltpu.VMEM((cols_n, own, features), BF16),
            pltpu.VMEM((tile_rows * heads, tile_cols), F32),
            pltpu.VMEM((heads, tile_rows, tile_cols), F32),
            pltpu.VMEM((lane_blocks, widest * tile_rows, LANES), BF16),
            pltpu.VMEM((heads * tile_cols, LANES), BF16),
            pltpu.VMEM((tile_rows, heads * tile_cols), BF16),
            pltpu.VMEM((lane_blocks, widest * tile_cols, LANES), BF16),
            pltpu.VMEM((cols_n, lane_blocks + 1, own, LANES), BF16),
            pltpu.VMEM((cols_n, lane_blocks + 1, own, LANES), BF16),
            dma((6,)),
            dma((chunks,)),
            dma((2, cols_n)),
            dma((cols_n,)),
            dma((rows_n,)),
            dma((rows_n,)),
            dma((cols_n,)),
            dma((cols_n,)),
            pltpu.SemaphoreType.REGULAR,
            pltpu.SemaphoreType.REGULAR,
            dma((cols_n,)),
            dma((cols_n,)),
            dma((cols_n,)),
        ],
        compiler_params=pltpu.CompilerParams(collective_id=0, has_side_effects=True),
    )(singles, pair, chain_sizes, single_proj, query_bias, pair_proj.T, out_proj)


def solution(mesh):
    placed = (
        P(("parts", "rows", "cols"), None),
        P(("parts", "rows"), "cols", None),
        P("parts"),
        P(),
        P(),
        P(),
        P(),
    )
    return jax.shard_map(
        functools.partial(shards, mesh.shape["rows"], mesh.shape["cols"]),
        mesh=mesh,
        in_specs=placed,
        out_specs=P(("parts", "rows", "cols"), None),
        check_vma=False,
    )
```

```python
import functools

import jax
import jax.numpy as jnp
from jax import lax
from jax.experimental import pallas as pl
from jax.experimental.pallas import tpu as pltpu
from jax.sharding import PartitionSpec as P

LANES = 128
MASKED = -1e30
FLOOR = -1e28
F32 = jnp.float32
BF16 = jnp.bfloat16


def peer(axis, index):
    return dict(device_id={axis: index}, device_id_type=pl.DeviceIdType.MESH)


def normalize(rows, axis):
    centered = rows - jnp.mean(rows, axis=axis, keepdims=True)
    variance = jnp.mean(centered * centered, axis=axis, keepdims=True)
    return centered * lax.rsqrt(variance + 1e-05)


def matmul(a, b):
    return jnp.dot(a, b, preferred_element_type=F32)


def iota(shape, dim):
    return lax.broadcasted_iota(jnp.int32, shape, dim)


def flat(blocks):
    count, rows, width = blocks.shape
    return blocks.astype(F32).reshape(count * rows, width).astype(BF16)


def kernel(
    rows_n,
    cols_n,
    chunks,
    singles,
    pair,
    chain,
    proj,
    q_bias,
    pair_proj,
    out_proj,
    out,
    own_v,
    pair_v,
    chain_s,
    proj_v,
    q_bias_v,
    pair_proj_v,
    out_proj_v,
    query_in,
    row_in,
    key_in,
    bias_v,
    score_v,
    stack_v,
    ones_v,
    weight_v,
    value_v,
    part_out,
    part_in,
    load_sem,
    pair_sem,
    query_send,
    query_recv,
    row_send,
    row_recv,
    key_send,
    key_recv,
    ready_up,
    ready_down,
    twin_send,
    part_send,
    part_recv,
):
    own, features = own_v.shape
    tile_rows, tile_cols, channels = pair_v.shape
    heads = pair_proj_v.shape[0]
    head_dim = features // heads
    lane_blocks = features // LANES
    slots = chain_s.shape[0]
    scale = head_dim ** (-0.5)
    row = lax.axis_index("rows")
    col = lax.axis_index("cols")

    loads = [
        pltpu.make_async_copy(src, dst, load_sem.at[n])
        for n, (src, dst) in enumerate(
            [
                (singles, own_v),
                (pair_proj, pair_proj_v),
                (proj, proj_v),
                (q_bias, q_bias_v.at[0]),
                (out_proj, out_proj_v),
                (chain, chain_s),
            ]
        )
    ]
    step = tile_rows // chunks

    def piece(n):
        rows = pl.ds(pl.multiple_of(n * step, step), step)
        return pltpu.make_async_copy(pair.at[rows], pair_v.at[rows], pair_sem.at[n])

    loads[0].start()
    loads[1].start()
    piece(0).start()
    for load in loads[2:]:
        load.start()
    for n in range(1, chunks):
        piece(n).start()

    reach = cols_n // 4
    core = lax.rem(row, 2)
    chips = rows_n // 2
    near = [d for n in range(reach, 0, -1) for d in (n, -n)]

    def along(d):
        return lax.rem(col + d + cols_n, cols_n)

    def across(d):
        return lax.rem(row + 2 * d, rows_n)

    def mine(target):
        return lax.rem(target, 2) == core

    barrier = pltpu.get_barrier_semaphore()
    for d in near:
        pl.semaphore_signal(barrier, inc=1, **peer("cols", along(d)))
    for d in range(1, chips):
        pl.semaphore_signal(barrier, inc=1, **peer("rows", across(d)))
    twin = row + 1 - 2 * core
    pl.semaphore_signal(barrier, inc=1, **peer("rows", twin))

    def send(src, dst, sent, arrived, axis, index):
        return pltpu.make_async_remote_copy(
            src_ref=src, dst_ref=dst, send_sem=sent, recv_sem=arrived, **peer(axis, index)
        )

    def query_copy(slot, target, stage):
        return send(
            query_in.at[slot],
            query_in.at[slot],
            query_send.at[stage, target],
            query_recv.at[slot],
            "cols",
            target,
        )

    def row_copy(target):
        return send(
            row_in.at[row], row_in.at[row], row_send.at[target], row_recv.at[row], "rows", target
        )

    def key_copy(src, slot, target):
        return send(
            row_in.at[src], key_in.at[slot], key_send.at[target], key_recv.at[slot], "cols", target
        )

    def twin_copy(slot):
        return send(
            key_in.at[slot], key_in.at[slot], twin_send.at[slot], key_recv.at[slot], "rows", twin
        )

    def part_copy(other):
        return send(
            part_out.at[other],
            part_in.at[col],
            part_send.at[other],
            part_recv.at[col],
            "cols",
            other,
        )

    def part_arrival(other):
        return send(
            part_in.at[other],
            part_in.at[other],
            part_send.at[other],
            part_recv.at[other],
            "cols",
            other,
        )

    def row_arrival(target):
        return send(
            row_in.at[target],
            row_in.at[target],
            row_send.at[target],
            row_recv.at[target],
            "rows",
            target,
        )

    def query_stage(act):
        for d in near:
            act(query_copy(col, along(d), 0))

    def query_relay(direction, act):
        for n in range(reach if direction > 0 else reach - 1, 0, -1):
            act(query_copy(along(-direction * reach), along(direction * n), 1))

    far_first = sorted(range(1, cols_n), key=lambda d: -min(d, cols_n - d))

    def key_stage(act, wait):
        def pass_on(target, copy):
            @pl.when(mine(target))
            def _():
                if wait:

                    @pl.when(target != row)
                    def _():
                        row_arrival(target).wait_recv()

                act(copy)

        if wait:
            pl.semaphore_wait(ready_up, 1)
            pl.semaphore_wait(ready_down, 1)
        for d in far_first:
            pass_on(along(d), key_copy(along(d), col, along(d)))

    def start(copy):
        copy.start()

    def wait_send(copy):
        copy.wait_send()


    loads[0].wait()
    normed = normalize(own_v[...].astype(F32), -1).astype(BF16)
    query_in[pl.ds(col, 1)] = normed[None]
    row_in[pl.ds(row, 1)] = normed[None]

    loads[1].wait()
    pair_w = pair_proj_v[...]

    def bias_chunks(first, last):
        @pl.loop(first, last)
        def _(n):
            piece(n).wait()
            for m in range(step):
                i = n * step + m
                block = jnp.transpose(pair_v[i]).astype(F32)
                bias = matmul(pair_w, normalize(block, 0).astype(BF16))
                bias_v[pl.ds(pl.multiple_of(i * heads, heads), heads), :] = bias.astype(BF16).astype(F32)

    bias_chunks(0, chunks // 4)
    pl.semaphore_wait(barrier, len(near) + chips)
    for d in range(1, chips):
        row_copy(across(d)).start()
    pl.semaphore_signal(ready_up, inc=1, **peer("cols", along(-reach)))
    pl.semaphore_signal(ready_down, inc=1, **peer("cols", along(reach)))
    query_stage(start)
    bias_chunks(chunks // 4, 5 * chunks // 8)

    key_stage(start, True)
    query_copy(along(-reach), along(-reach), 0).wait_recv()
    query_relay(1, start)
    query_copy(along(reach), along(reach), 0).wait_recv()
    query_relay(-1, start)

    @pl.when(mine(col))
    def _():
        @pl.when(col != row)
        def _():
            row_arrival(col).wait_recv()

        key_in[pl.ds(col, 1)] = row_in[pl.ds(col, 1)]

    loads[2].wait()
    loads[3].wait()
    own_gate = jax.nn.sigmoid(matmul(normed, proj_v[:, 3 * features :]))
    bias_chunks(5 * chunks // 8, chunks)

    def blocks_of(h):
        return range(h * head_dim // LANES, ((h + 1) * head_dim - 1) // LANES + 1)

    def head_lanes(b, h):
        feature = iota((1, LANES), 1) + b * LANES
        return (feature >= h * head_dim) & (feature < (h + 1) * head_dim)

    def lanes_of(b):
        return slice(b * LANES, (b + 1) * LANES)

    members = [[h for h in range(heads) if b in blocks_of(h)] for b in range(lane_blocks)]
    fresh = [[h for h in members[b] if blocks_of(h)[0] == b] for b in range(lane_blocks)]
    crossing = [[h for h in fresh[b] if blocks_of(h)[-1] > b] for b in range(lane_blocks)]

    loads[5].wait()
    live = chain_s[0]
    for n in range(1, slots - 1):
        live = live + chain_s[n]
    key_live = iota((1, tile_cols), 1) + col * tile_cols < live
    lane = iota((1, LANES), 1)
    ones_head = lax.div(iota((heads * tile_cols, LANES), 0), tile_cols)
    ones_lane = iota((heads * tile_cols, LANES), 1)
    ones_v[...] = jnp.where(
        (lax.rem(ones_lane, heads) == ones_head) & (ones_lane < 2 * heads), 1.0, 0.0
    ).astype(BF16)
    for h in range(heads):
        score_v[h] = jnp.where(key_live, bias_v[pl.ds(h, tile_rows, stride=heads), :], MASKED)

    for d in far_first:
        if d not in (reach, cols_n - reach):
            query_copy(along(d), along(d), 0).wait_recv()
    queries = (
        matmul(flat(query_in[...]), proj_v[:, :features]) + q_bias_v[...]
    ).astype(BF16).astype(F32)
    for b in range(lane_blocks):
        for n, h in enumerate(fresh[b]):
            stack_v[b, n * tile_rows : (n + 1) * tile_rows, :] = jnp.where(
                head_lanes(b, h), queries[:, lanes_of(b)], 0.0
            ).astype(BF16)
        for n, h in enumerate(crossing[b], len(fresh[b])):
            stack_v[b, n * tile_rows : (n + 1) * tile_rows, :] = jnp.where(
                head_lanes(b + 1, h), queries[:, lanes_of(b + 1)], 0.0
            ).astype(BF16)

    @pl.when(mine(col))
    def _():
        twin_copy(col).start()
        for d in reversed(far_first):
            key_copy(along(d), along(d), along(d)).wait_recv()
            twin_copy(along(d)).start()

    @pl.when(jnp.logical_not(mine(col)))
    def _():
        for d in range(cols_n):
            twin_copy(along(d)).wait_recv()

    key_side = matmul(flat(key_in[...]), proj_v[:, features : 3 * features]).astype(BF16)
    keys = key_side[:, :features]
    values = key_side[:, features:].astype(F32)

    def against_keys(stacked, b):
        return lax.dot_general(
            stacked, keys[:, lanes_of(b)], (((1,), (1,)), ((), ())), preferred_element_type=F32
        )

    own_rows = tile_rows // cols_n
    top = jnp.zeros((tile_rows, LANES), F32)
    summed_weights = jnp.zeros((tile_rows, LANES), F32)
    for b in range(lane_blocks):
        count = len(fresh[b])
        raw = against_keys(stack_v[b, : count * tile_rows, :], b)
        if crossing[b]:
            extra = against_keys(
                stack_v[b, count * tile_rows : (count + len(crossing[b])) * tile_rows, :], b + 1
            )
        for n, h in enumerate(fresh[b]):
            scores = raw[n * tile_rows : (n + 1) * tile_rows]
            if h in crossing[b]:
                at = crossing[b].index(h) * tile_rows
                scores = scores + extra[at : at + tile_rows]
            score_v[h] = scores * scale + score_v[h]
        for n, h in enumerate(members[b]):
            value_v[b, n * tile_cols : (n + 1) * tile_cols, :] = jnp.where(
                head_lanes(b, h), values[:, lanes_of(b)], 0.0
            ).astype(BF16)
    for b in range(lane_blocks):
        for h in fresh[b]:
            scores = score_v[h]
            largest = jnp.maximum(jnp.max(scores, axis=-1, keepdims=True), FLOOR)
            weight_v[:, h * tile_cols : (h + 1) * tile_cols] = jnp.exp(scores - largest).astype(BF16)
            top = jnp.where(lax.rem(lane, heads) == h, largest, top)
    for b in range(lane_blocks):
        summed = matmul(
            weight_v[:, members[b][0] * tile_cols : (members[b][-1] + 1) * tile_cols],
            value_v[b, : len(members[b]) * tile_cols, :],
        )
        part_out[:, b] = summed.reshape(cols_n, own_rows, LANES).astype(BF16)
        span = slice(fresh[b][0] * tile_cols, (fresh[b][-1] + 1) * tile_cols)
        summed_weights = summed_weights + matmul(weight_v[:, span], ones_v[span, :])

    stats = jnp.where(lane < 2 * heads, summed_weights, top)
    first = stats.astype(BF16).astype(F32)
    second = (stats - first).astype(BF16).astype(F32)
    third = stats - first - second
    group = lax.div(lane, heads)
    stats = jnp.where(
        (group == 0) | (group == 2), first, jnp.where((group == 1) | (group == 3), second, third)
    )
    stats = jnp.where(group < 5, stats, 0.0)
    part_out[:, lane_blocks] = stats.reshape(cols_n, own_rows, LANES).astype(BF16)
    for d in far_first:
        part_copy(along(d)).start()
    part_in[pl.ds(col, 1)] = part_out[pl.ds(col, 1)]
    loads[4].wait()
    spread_row = iota((LANES, features), 0)
    spread_head = lax.div(iota((LANES, features), 1), head_dim)
    matches = lax.rem(spread_row, heads) == spread_head
    spread_group = lax.div(spread_row, heads)
    to_total = jnp.where(matches & (spread_group < 2), 1.0, 0.0).astype(BF16)
    to_top = jnp.where(matches & (spread_group >= 2) & (spread_group < 5), 1.0, 0.0).astype(BF16)
    for d in far_first:
        part_arrival(along(d)).wait_recv()
    arrived = flat(part_in[:, lane_blocks])
    total = matmul(arrived, to_total).reshape(cols_n, own_rows, features)
    tops = matmul(arrived, to_top).reshape(cols_n, own_rows, features)
    factor = jnp.exp(tops - jnp.max(tops, axis=0, keepdims=True))
    total = jnp.sum(factor * total, axis=0)
    numerator = jnp.concatenate(
        [
            jnp.sum(factor[:, :, lanes_of(b)] * part_in[:, b].astype(F32), axis=0)
            for b in range(lane_blocks)
        ],
        axis=-1,
    )
    attended = (own_gate * (numerator / total)).astype(BF16)
    out[...] = matmul(attended, out_proj_v[...]).astype(BF16)

    for d in range(1, chips):
        row_copy(across(d)).wait_send()
    query_stage(wait_send)
    query_relay(1, wait_send)
    query_relay(-1, wait_send)
    key_stage(wait_send, False)

    @pl.when(mine(col))
    def _():
        for d in range(cols_n):
            twin_copy(along(d)).wait_send()

    for d in far_first:
        part_copy(along(d)).wait_send()


def shards(rows_n, cols_n, singles, pair, chain_sizes, single_proj, query_bias, pair_proj, out_proj):
    own, features = singles.shape
    tile_rows, tile_cols, channels = pair.shape
    heads = pair_proj.shape[1]
    chunks = 8
    dma = pltpu.SemaphoreType.DMA
    lane_blocks = features // LANES
    widest = -(-LANES // (features // heads)) + 1
    return pl.pallas_call(
        functools.partial(kernel, rows_n, cols_n, chunks),
        out_shape=pltpu.VMEM((own, features), BF16),
        in_specs=[pl.BlockSpec(memory_space=pl.ANY)] * 7,
        out_specs=pl.BlockSpec(memory_space=pltpu.VMEM),
        scratch_shapes=[
            pltpu.VMEM((own, features), BF16),
            pltpu.VMEM(pair.shape, BF16),
            pltpu.SMEM(chain_sizes.shape, jnp.int32),
            pltpu.VMEM(single_proj.shape, BF16),
            pltpu.VMEM((1, features), F32),
            pltpu.VMEM((heads, channels), BF16),
            pltpu.VMEM(out_proj.shape, BF16),
            pltpu.VMEM((cols_n, own, features), BF16),
            pltpu.VMEM((rows_n, own, features), BF16),
            pltpu.VMEM((cols_n, own, features), BF16),
            pltpu.VMEM((tile_rows * heads, tile_cols), F32),
            pltpu.VMEM((heads, tile_rows, tile_cols), F32),
            pltpu.VMEM((lane_blocks, widest * tile_rows, LANES), BF16),
            pltpu.VMEM((heads * tile_cols, LANES), BF16),
            pltpu.VMEM((tile_rows, heads * tile_cols), BF16),
            pltpu.VMEM((lane_blocks, widest * tile_cols, LANES), BF16),
            pltpu.VMEM((cols_n, lane_blocks + 1, own, LANES), BF16),
            pltpu.VMEM((cols_n, lane_blocks + 1, own, LANES), BF16),
            dma((6,)),
            dma((chunks,)),
            dma((2, cols_n)),
            dma((cols_n,)),
            dma((rows_n,)),
            dma((rows_n,)),
            dma((cols_n,)),
            dma((cols_n,)),
            pltpu.SemaphoreType.REGULAR,
            pltpu.SemaphoreType.REGULAR,
            dma((cols_n,)),
            dma((cols_n,)),
            dma((cols_n,)),
        ],
        compiler_params=pltpu.CompilerParams(collective_id=0, has_side_effects=True),
    )(singles, pair, chain_sizes, single_proj, query_bias, pair_proj.T, out_proj)


def solution(mesh):
    placed = (
        P(("parts", "rows", "cols"), None),
        P(("parts", "rows"), "cols", None),
        P("parts"),
        P(),
        P(),
        P(),
        P(),
    )
    return jax.shard_map(
        functools.partial(shards, mesh.shape["rows"], mesh.shape["cols"]),
        mesh=mesh,
        in_specs=placed,
        out_specs=P(("parts", "rows", "cols"), None),
        check_vma=False,
    )
```
